256 devices in a mesh: veh: 64 (over z, y, core), row: 4 (over x).
Axes of the slice: x: 4, y: 4, z: 8, core: 2. Of those that a mesh axis runs over, the one named last changes fastest.
Arguments:
- bev_maps: bfloat16 [512, 32, 64, 128], P('veh', 'row'), may hold values from -6 to 6
- senders: int32 [512, 4], replicated, may hold values from 0 to 511, as said below
- shifts: int32 [512, 4], replicated, may hold values from -1 to 1
- counts: int32 [512], replicated, may hold values from 1 to 4, as said below
- agent_query: bfloat16 [128, 128], replicated, may hold values from -0.5 to 0.5
- agent_keyvalue: bfloat16 [128, 256], replicated, may hold values from -0.5 to 0.5
- agent_out: bfloat16 [128, 128], replicated, may hold values from -0.5 to 0.5
- agent_scale: float32 [4], replicated, may hold values from 1 to 600
- conv_weight: float32 [3, 3, 256], replicated, may hold values from -1.5 to 1.5
- gain_first: float32 [256], replicated, may hold values from 0.1 to 1.9
- window_in: bfloat16 [256, 768], replicated, may hold values from -0.375 to 0.375
- window_out: bfloat16 [256, 256], replicated, may hold values from -0.375 to 0.375
- window_scale: float32 [8], replicated, may hold values from 1 to 600
- gain_second: float32 [256], replicated, may hold values from 0.1 to 1.9
- hidden_up: bfloat16 [256, 512], replicated, may hold values from -0.375 to 0.375
- hidden_down: bfloat16 [512, 256], replicated, may hold values from -0.25 to 0.25
Outputs:
- joined_map: bfloat16 [512, 32, 64, 256], P('veh', 'row')
The draws below stay inside these ranges and needn't reach their ends.
Inputs may be any that keep to these rules, and one draw needn't show every extreme that they name: `senders`: never the receiver itself. Blocks are aligned runs of 8 vehicles; over the live pairs whose receiver lies in one block and whose sender lies in one block, the intersecting tiles (2 - |shift| a pair) number at most 2. Slots a < counts[r] of receiver r are live.
All inputs are finite; a program needn't handle non-finite values.
Results may differ from the reference program's by a relative error of at most 0.0095.
The reference program's roundings to bfloat16 on the way count: a program that leaves them out, or rounds other values in their place, can miss the bound.
Values may be sent and summed in bfloat16 or wider, within the bound.
A program may use at most 128 MiB of HBM per device.

```python
import math
import jax
import jax.numpy as jnp
from jax import lax

VEH_DEV = 8
AGENTS = 4
CH = 128
WIDTH = 256
HEADS = 8
AGENT_HEADS = 4
MLP = 512
TILE = 32
WIN = 8
MAP_COLS = 64
MAP_ROWS = 32
VEHICLES = 512


def pair_tables(key):
    base_key = jax.random.fold_in(key, 101)
    order_key, local_key, shift_key, count_key, full_key, zero_key, keep_key = jax.random.split(base_key, 7)
    devices = VEHICLES // VEH_DEV
    pair_count = AGENTS * VEH_DEV
    domain = max(devices, pair_count)
    tile_cols = MAP_COLS // TILE
    device_keys = jax.random.split(order_key, devices)
    orders = jax.vmap(lambda single_key: jax.random.permutation(single_key, domain))(device_keys)[:, :pair_count]
    receiver_dev = jnp.arange(devices, dtype=jnp.int32)[:, None]
    source_dev = (receiver_dev + orders % devices) % devices
    local_pick = jax.random.randint(local_key, (devices, pair_count), 0, VEH_DEV)
    receiver_local = (jnp.arange(pair_count, dtype=jnp.int32) // AGENTS)[None, :]
    clash = (source_dev == receiver_dev) & (local_pick == receiver_local)
    local_pick = jnp.where(clash, (local_pick + 1) % VEH_DEV, local_pick)
    senders = (source_dev * VEH_DEV + local_pick).reshape(VEHICLES, AGENTS).astype(jnp.int32)
    shifts = jax.random.randint(shift_key, (VEHICLES, AGENTS), 1 - tile_cols, tile_cols)
    zero_pick = jax.random.randint(zero_key, (VEHICLES, AGENTS), 0, 2) == 0
    shifts = jnp.where(zero_pick, 0, shifts)
    counts = jax.random.randint(count_key, (VEHICLES,), 1, AGENTS + 1)
    keep_full = jax.random.randint(keep_key, (VEHICLES,), 0, 4) != 0
    counts = jnp.where(keep_full, AGENTS, counts)
    full_dev = jax.random.randint(full_key, (), 0, devices)
    on_full = jnp.arange(VEHICLES, dtype=jnp.int32) // VEH_DEV == full_dev
    counts = jnp.where(on_full, AGENTS, counts).astype(jnp.int32)
    shifts = jnp.where(on_full[:, None], 0, shifts).astype(jnp.int32)
    return (senders, shifts, counts)


def draw_senders(key, part):
    return pair_tables(key)[0]


def draw_shifts(key, part):
    return pair_tables(key)[1]


def draw_counts(key, part):
    return pair_tables(key)[2]


def head_scales(key, count, salt):
    salted = jax.random.fold_in(key, salt)
    first_key = jax.random.fold_in(salted, 0)
    scales = jnp.exp(jax.random.uniform(first_key, (count,), jnp.float32, 0.0, math.log(40.0)))
    return scales.astype(jnp.float32)


def draw_agent_scale(key, part):
    return head_scales(key, AGENT_HEADS, 211)


def draw_window_scale(key, part):
    return head_scales(key, HEADS, 223)


def level_of(key, shape, shards, smallest, high):
    factor_of, own = 1.0, jax.random.fold_in(key, 6)
    for axis_at, shards_of in shards:
        draws = jnp.exp(jax.random.uniform(jax.random.fold_in(own, axis_at), (shards_of,), jnp.float32, smallest / len(shards), high / len(shards)))
        factor_of = factor_of * jnp.repeat(draws, shape[axis_at] // shards_of).reshape([-1 if axis == axis_at else 1 for axis in range(len(shape))])
    return factor_of


def scatter_about(rng, shape, scale, reach, pieces=(), held_as=jnp.bfloat16):
    entries = scale * jax.random.normal(rng, shape, jnp.float32)
    if pieces:
        entries = entries * level_of(rng, shape, pieces, -0.22, 0.18)
    return jnp.clip(entries, -reach, reach).astype(held_as)


def setup_inputs(seed: int = 0) -> dict:
    seeds = jax.random.split(jax.random.key(seed), 17)
    return {
        "bev_maps": scatter_about(seeds[0], (VEHICLES, MAP_ROWS, MAP_COLS, CH), 1.0, 6.0, ((0, 64), (1, 4))),
        "senders": draw_senders(jax.random.fold_in(seeds[16], 71), 0),
        "shifts": draw_shifts(jax.random.fold_in(seeds[16], 71), 0),
        "counts": draw_counts(jax.random.fold_in(seeds[16], 71), 0),
        "agent_query": scatter_about(seeds[4], (CH, CH), CH ** -0.5, 0.5),
        "agent_keyvalue": scatter_about(seeds[5], (CH, 2 * CH), CH ** -0.5, 0.5),
        "agent_out": scatter_about(seeds[6], (CH, CH), CH ** -0.5, 0.5),
        "agent_scale": draw_agent_scale(jax.random.fold_in(seeds[16], 71), 0),
        "conv_weight": scatter_about(seeds[8], (3, 3, WIDTH), 0.3, 1.5, (), jnp.float32),
        "gain_first": jnp.clip(1.0 + 0.18 * jax.random.normal(seeds[9], (WIDTH,), jnp.float32), 0.1, 1.9),
        "window_in": scatter_about(seeds[10], (WIDTH, 3 * WIDTH), WIDTH ** -0.5, 0.375),
        "window_out": scatter_about(seeds[11], (WIDTH, WIDTH), WIDTH ** -0.5, 0.375),
        "window_scale": draw_window_scale(jax.random.fold_in(seeds[16], 71), 0),
        "gain_second": jnp.clip(1.0 + 0.18 * jax.random.normal(seeds[13], (WIDTH,), jnp.float32), 0.1, 1.9),
        "hidden_up": scatter_about(seeds[14], (WIDTH, MLP), WIDTH ** -0.5, 0.375),
        "hidden_down": scatter_about(seeds[15], (MLP, WIDTH), MLP ** -0.5, 0.25),
    }


exact_dot = lax.Precision.HIGHEST
norm_eps = 1e-05
unit_eps = 1e-06

def head_spread(tensor, head_count):
    feature_width = tensor.shape[-1]
    member = (jnp.arange(feature_width)[:, None] // (feature_width // head_count) == jnp.arange(head_count)[None, :]).astype(jnp.float32)
    summed = jnp.dot(tensor, member, precision=exact_dot)
    return jnp.dot(summed, member.T, precision=exact_dot)

def unit_heads(tensor, head_count):
    return tensor / jnp.sqrt(head_spread(tensor * tensor, head_count) + unit_eps)

def join_agents(ego_map, own_keyvalue, sent_keyvalue, covered, agent_query, agent_out, agent_scale):
    channels = ego_map.shape[-1]
    head_count = agent_scale.shape[0]
    queries = unit_heads(jnp.dot(ego_map, agent_query, preferred_element_type=jnp.float32), head_count)
    all_kv = jnp.concatenate([own_keyvalue[:, None], sent_keyvalue], axis=1).astype(jnp.float32)
    key_part = unit_heads(all_kv[..., :channels], head_count)
    values = all_kv[..., channels:]
    scale_row = jnp.repeat(agent_scale, channels // head_count)
    scores = head_spread(queries[:, None] * key_part, head_count) * scale_row
    present = jnp.concatenate([jnp.ones_like(covered[:, :1]), covered], axis=1)[..., None]
    scores = jnp.where(present, scores, -1e+30)
    row_top = lax.optimization_barrier(jnp.max(scores, axis=1, keepdims=True))
    weight = jnp.where(present, jnp.exp(scores - row_top), 0.0)
    weight = weight / lax.optimization_barrier(jnp.sum(weight, axis=1, keepdims=True))
    agent_mix = lax.optimization_barrier(jnp.sum(weight * values, axis=1)).astype(jnp.bfloat16)
    joined = jnp.dot(agent_mix, agent_out, preferred_element_type=jnp.float32).astype(jnp.bfloat16)
    return jnp.concatenate([ego_map, joined], axis=-1)

def layer_norm(tensor, gain):
    average = lax.optimization_barrier(jnp.mean(tensor, axis=-1, keepdims=True))
    centred = tensor - average
    spread = lax.optimization_barrier(jnp.mean(centred * centred, axis=-1, keepdims=True))
    return centred * lax.rsqrt(spread + norm_eps) * gain

def to_windows(tensor, head_count):
    batch_size, height, width_cells, feature_width = tensor.shape
    tensor = tensor.reshape(batch_size, height // WIN, WIN, width_cells // WIN, WIN, head_count, feature_width // head_count)
    tensor = tensor.transpose(0, 1, 3, 5, 2, 4, 6)
    return tensor.reshape(batch_size, height // WIN, width_cells // WIN, head_count, WIN * WIN, feature_width // head_count)

def from_windows(tensor, height, width_cells):
    batch_size = tensor.shape[0]
    head_count = tensor.shape[3]
    head_width = tensor.shape[-1]
    tensor = tensor.reshape(batch_size, height // WIN, width_cells // WIN, head_count, WIN, WIN, head_width)
    tensor = tensor.transpose(0, 1, 4, 2, 5, 3, 6)
    return tensor.reshape(batch_size, height, width_cells, head_count * head_width)

def window_layer(padded, conv_weight, gain_first, window_in, window_out, window_scale, gain_second, hidden_up, hidden_down):
    batch_size, height, width_cells, feature_width = padded.shape
    height = height - 2
    widened = jnp.pad(padded, ((0, 0), (0, 0), (1, 1), (0, 0))).astype(jnp.float32)
    mixed_sum = widened[:, 1:height + 1, 1:width_cells + 1]
    for row_step in range(3):
        for col_step in range(3):
            mixed_sum = mixed_sum + widened[:, row_step:row_step + height, col_step:col_step + width_cells] * conv_weight[row_step, col_step]
    hidden = layer_norm(mixed_sum, gain_first).astype(jnp.bfloat16)
    projected = jnp.dot(hidden, window_in, preferred_element_type=jnp.float32)
    head_count = window_scale.shape[0]
    queries = to_windows(unit_heads(projected[..., :feature_width], head_count), head_count)
    key_part = to_windows(unit_heads(projected[..., feature_width:2 * feature_width], head_count), head_count)
    values = to_windows(projected[..., 2 * feature_width:].astype(jnp.bfloat16), head_count)
    scores = jnp.einsum('bxyhqd,bxyhkd->bxyhqk', queries, key_part, precision=exact_dot) * window_scale[:, None, None]
    row_top = lax.optimization_barrier(jnp.max(scores, axis=-1, keepdims=True))
    weight = jnp.exp(scores - row_top)
    weight = (weight / lax.optimization_barrier(jnp.sum(weight, axis=-1, keepdims=True))).astype(jnp.bfloat16)
    attended = jnp.einsum('bxyhqk,bxyhkd->bxyhqd', weight.astype(jnp.float32), values.astype(jnp.float32), precision=exact_dot)
    attended = from_windows(attended, height, width_cells).astype(jnp.bfloat16)
    mixed_sum = mixed_sum + jnp.dot(attended, window_out, preferred_element_type=jnp.float32)
    hidden = layer_norm(mixed_sum, gain_second).astype(jnp.bfloat16)
    inner_act = jax.nn.silu(jnp.dot(hidden, hidden_up, preferred_element_type=jnp.float32)).astype(jnp.bfloat16)
    return (mixed_sum + jnp.dot(inner_act, hidden_down, preferred_element_type=jnp.float32)).astype(jnp.bfloat16)

def reference(bev_maps, senders, shifts, counts, agent_query, agent_keyvalue, agent_out, agent_scale, conv_weight, gain_first, window_in, window_out, window_scale, gain_second, hidden_up, hidden_down):
    vehicles, height, width_cells, channels = bev_maps.shape
    agents = senders.shape[1]
    tile_cols = width_cells // TILE
    cell_count = height * width_cells
    blocked = bev_maps.reshape(vehicles // 4, 4, height, width_cells, channels)
    key_values = lax.map(lambda group_maps: jnp.dot(group_maps, agent_keyvalue, preferred_element_type=jnp.float32).astype(jnp.bfloat16), blocked)
    flat_kv = key_values.reshape(vehicles, height, width_cells, 2 * channels)
    tile_of = jnp.arange(width_cells) // TILE

    def one_group(operands):
        group_maps, group_kv, group_senders, group_shifts, group_counts = operands
        group_size = group_maps.shape[0]
        sent_keyvalue = jnp.take(flat_kv, group_senders.reshape(-1), axis=0)
        shift_flat = group_shifts.reshape(-1)
        sent_keyvalue = jax.vmap(lambda plane_kv, amount: jnp.roll(plane_kv, -amount * TILE, axis=1))(sent_keyvalue, shift_flat)
        shifted = tile_of[None, :] + shift_flat[:, None]
        present_pair = (jnp.arange(agents)[None, :] < group_counts[:, None]).reshape(-1)
        covered = (shifted >= 0) & (shifted < tile_cols) & present_pair[:, None]
        covered = jnp.broadcast_to(covered.reshape(group_size, agents, 1, width_cells), (group_size, agents, height, width_cells)).reshape(group_size, agents, cell_count)
        mixed_in = join_agents(group_maps.reshape(group_size, cell_count, channels), group_kv.reshape(group_size, cell_count, 2 * channels), sent_keyvalue.reshape(group_size, agents, cell_count, 2 * channels), covered, agent_query, agent_out, agent_scale)
        padded = jnp.pad(mixed_in.reshape(group_size, height, width_cells, 2 * channels), ((0, 0), (1, 1), (0, 0), (0, 0)))
        return window_layer(padded, conv_weight, gain_first, window_in, window_out, window_scale, gain_second, hidden_up, hidden_down)
    result = lax.map(one_group, (blocked, key_values, senders.reshape(vehicles // 4, 4, agents), shifts.reshape(vehicles // 4, 4, agents), counts.reshape(vehicles // 4, 4)))
    return result.reshape(vehicles, height, width_cells, 2 * channels)
```

```python
import functools
import jax
import jax.numpy as jnp
from jax import lax
from jax.experimental import pallas as pl
from jax.experimental.pallas import tpu as pltpu
from jax.sharding import PartitionSpec as P

TILE = 32
WIN = 8
HEAD = 32
norm_eps = 1e-05
unit_eps = 1e-06
f32 = jnp.float32
bf16 = jnp.bfloat16


def nt_dot(a, b):
    return lax.dot_general(a, b, (((1,), (1,)), ((), ())), preferred_element_type=f32)


def halves(x):
    high = x.astype(bf16)
    return high, (x - high.astype(f32)).astype(bf16)


def head_sums(x, member):
    return jnp.dot(jnp.concatenate(halves(x), axis=-1), member, preferred_element_type=f32)


def agent_kernel(slot_ref, live_ref, ego_ref, t0, t1, t2, t3, query_ref, keyvalue_ref, out_w_ref,
                 scale_ref, member_ref, joined_ref):
    step = pl.program_id(0)
    tiles = (t0, t1, t2, t3)
    height, cols, channels = ego_ref.shape[1:]
    cells = height * cols
    ego = ego_ref[0].reshape(cells, channels)
    member = member_ref[...]
    query = jnp.dot(ego, query_ref[...], preferred_element_type=f32)
    query = query * (lax.rsqrt(head_sums(query * query, member) + unit_eps) * scale_ref[...])
    scores, values = [], []
    for a in range(len(tiles) + 1):
        source = ego if a == 0 else tiles[a - 1][0].reshape(cells, channels)
        keyvalue = jnp.dot(source, keyvalue_ref[...], preferred_element_type=f32).astype(bf16)
        key = keyvalue[:, :channels].astype(f32)
        values.append(keyvalue[:, channels:])
        score = head_sums(query * key, member) * lax.rsqrt(head_sums(key * key, member) + unit_eps)
        if a:
            score = score + jnp.where(live_ref[step * len(tiles) + a - 1] > 0, 0.0, -1e30)
        scores.append(score)
    top = functools.reduce(jnp.maximum, scores)
    total, mix = None, None
    for score, value in zip(scores, values):
        weight = jnp.exp(score - top)
        total = weight if total is None else total + weight
        part = weight * value.astype(f32)
        mix = part if mix is None else mix + part
    mix = (mix / total).astype(bf16)
    joined = jnp.dot(mix, out_w_ref[...], preferred_element_type=f32).astype(bf16)
    joined_ref[0] = joined.reshape(height, cols, channels)


def member_matrix(width):
    rows = jnp.arange(2 * width)[:, None] % width // HEAD
    return (rows == jnp.arange(width)[None, :] // HEAD).astype(bf16)


def agent_stage(bev_maps, arrived, slots, live, agent_query, agent_keyvalue, agent_out, agent_scale):
    vehicles, height, width_cells, channels = bev_maps.shape
    tile_cols = width_cells // TILE
    agents = slots.shape[1]
    full = lambda i, *_: (0, 0)
    ego_spec = pl.BlockSpec((1, height, TILE, channels), lambda i, *_: (i // tile_cols, 0, i % tile_cols, 0))
    tile_specs = [
        pl.BlockSpec((1, height, TILE, channels), lambda i, s, l, a=a: (s[i * agents + a], 0, 0, 0))
        for a in range(agents)
    ]
    scale_row = jnp.repeat(agent_scale, channels // agent_scale.shape[0])[None]
    return pl.pallas_call(
        agent_kernel,
        grid_spec=pltpu.PrefetchScalarGridSpec(
            num_scalar_prefetch=2,
            grid=(vehicles * tile_cols,),
            in_specs=[ego_spec, *tile_specs]
            + [pl.BlockSpec(w.shape, full) for w in (agent_query, agent_keyvalue, agent_out)]
            + [pl.BlockSpec((1, channels), full), pl.BlockSpec((2 * channels, channels), full)],
            out_specs=ego_spec,
        ),
        out_shape=jax.ShapeDtypeStruct(bev_maps.shape, bf16),
        compiler_params=pltpu.CompilerParams(dimension_semantics=("arbitrary",)),
        name="agent_stage",
    )(slots.reshape(-1), live.reshape(-1), bev_maps, arrived, arrived, arrived, arrived, agent_query,
      agent_keyvalue, agent_out, scale_row, member_matrix(channels))


def layer_norm(x, gain):
    centred = x - jnp.mean(x, axis=-1, keepdims=True)
    spread = jnp.mean(centred * centred, axis=-1, keepdims=True)
    return (centred * lax.rsqrt(spread + norm_eps) * gain).astype(bf16)


def layer_kernel(bev_ref, joined_ref, bev_up, bev_down, joined_up, joined_down, conv_ref, gain1_ref,
                 in_ref, out_w_ref, scale_ref, gain2_ref, up_ref, down_ref, member_ref, out_ref,
                 mixed_ref, attended_ref):
    height, cols, channels = bev_ref.shape[1:]
    cells = height * cols
    windows = cols // WIN
    area = WIN * WIN
    width = 2 * channels
    column = lax.broadcasted_iota(jnp.int32, (cells, channels), 0) % cols
    for half, (main, top, bottom) in enumerate(
        ((bev_ref, bev_up, bev_down), (joined_ref, joined_up, joined_down))
    ):
        lanes = slice(half * channels, (half + 1) * channels)
        rows = jnp.concatenate([top[0], main[0], bottom[0]], axis=0).astype(f32)
        sums = []
        for dj in range(3):
            taps = [conv_ref[di * 3 + dj : di * 3 + dj + 1, lanes] for di in range(3)]
            if dj == 1:
                taps[1] = taps[1] + 1.0
            acc = rows[0:height] * taps[0] + rows[1 : height + 1] * taps[1] + rows[2:] * taps[2]
            sums.append(acc.reshape(cells, channels))
        mixed = (
            sums[1]
            + jnp.where(column == 0, 0.0, pltpu.roll(sums[0], 1, axis=0))
            + jnp.where(column == cols - 1, 0.0, pltpu.roll(sums[2], cells - 1, axis=0))
        )
        for r in range(height):
            for w in range(windows):
                mixed_ref[w * area + r * WIN : w * area + (r + 1) * WIN, lanes] = mixed[
                    r * cols + w * WIN : r * cols + (w + 1) * WIN
                ]
    mixed = mixed_ref[...]
    hidden = layer_norm(mixed, gain1_ref[...])
    projected = jnp.dot(hidden, in_ref[...], preferred_element_type=f32)
    member = member_ref[...]
    groups = []
    for g in range(width // channels):
        lanes = slice(g * channels, (g + 1) * channels)
        query = projected[:, g * channels : (g + 1) * channels]
        key = projected[:, width + g * channels : width + (g + 1) * channels]
        query = query * (lax.rsqrt(head_sums(query * query, member) + unit_eps) * scale_ref[:, lanes])
        key = key * lax.rsqrt(head_sums(key * key, member) + unit_eps)
        value = projected[:, 2 * width + g * channels : 2 * width + (g + 1) * channels].astype(bf16)
        groups.append((jnp.concatenate(halves(query), axis=-1), *halves(key), value))
    heads = channels // HEAD
    head_of = lax.broadcasted_iota(jnp.int32, (area, 2 * channels), 1) % channels // HEAD
    lane_head = lax.broadcasted_iota(jnp.int32, (area, channels), 1) // HEAD
    for w in range(windows):
        span = slice(w * area, (w + 1) * area)
        for g, (query, key_high, key_low, value) in enumerate(groups):
            q = query[span]
            spread_q = jnp.concatenate(
                [jnp.where(head_of == j, q, jnp.zeros_like(q)) for j in range(heads)], axis=0
            )
            kh = key_high[span]
            scores = nt_dot(jnp.concatenate([kh, kh], axis=-1), spread_q) + nt_dot(
                key_low[span], spread_q[:, :channels]
            )
            weight = jnp.exp(scores - jnp.max(scores, axis=0, keepdims=True))
            weight = weight * (1.0 / jnp.sum(weight, axis=0, keepdims=True))
            mixed_values = jnp.dot(weight.T.astype(bf16), value[span], preferred_element_type=f32)
            attended = jnp.where(lane_head == 0, mixed_values[:area], 0.0)
            for j in range(1, heads):
                attended = jnp.where(lane_head == j, mixed_values[j * area : (j + 1) * area], attended)
            attended_ref[span, g * channels : (g + 1) * channels] = attended.astype(bf16)
    mixed = mixed + jnp.dot(attended_ref[...], out_w_ref[...], preferred_element_type=f32)
    hidden = layer_norm(mixed, gain2_ref[...])
    inner = jnp.dot(hidden, up_ref[...], preferred_element_type=f32)
    inner = (inner / (1.0 + jnp.exp(-inner))).astype(bf16)
    result = mixed + jnp.dot(inner, down_ref[...], preferred_element_type=f32)
    for r in range(height):
        for w in range(0, windows, 2):
            pair = [result[v * area + r * WIN : v * area + (r + 1) * WIN] for v in (w, w + 1)]
            out_ref[0, r, w * WIN : (w + 2) * WIN, :] = jnp.concatenate(pair, axis=0).astype(bf16)


def layer_stage(bev_maps, joined, bev_halo, joined_halo, conv_weight, gain_first, window_in, window_out,
                window_scale, gain_second, hidden_up, hidden_down):
    vehicles, height, width_cells, channels = bev_maps.shape
    width = 2 * channels
    cells = height * width_cells
    block = pl.BlockSpec((1, height, width_cells, channels), lambda i: (i, 0, 0, 0))
    edge = pl.BlockSpec((1, 1, width_cells, channels), lambda i: (i, 0, 0, 0))
    small = (
        conv_weight.reshape(9, width),
        gain_first[None],
        window_in,
        window_out,
        jnp.repeat(window_scale, width // window_scale.shape[0])[None],
        gain_second[None],
        hidden_up,
        hidden_down,
        member_matrix(channels),
    )
    return pl.pallas_call(
        layer_kernel,
        grid=(vehicles,),
        in_specs=[block, block, edge, edge, edge, edge]
        + [pl.BlockSpec(w.shape, lambda i: (0, 0)) for w in small],
        out_specs=pl.BlockSpec((1, height, width_cells, width), lambda i: (i, 0, 0, 0)),
        out_shape=jax.ShapeDtypeStruct((vehicles, height, width_cells, width), bf16),
        scratch_shapes=[pltpu.VMEM((cells, width), f32), pltpu.VMEM((cells, width), bf16)],
        compiler_params=pltpu.CompilerParams(dimension_semantics=("arbitrary",)),
        name="layer_stage",
    )(bev_maps, joined, *bev_halo, *joined_halo, *small)


def pack_kernel(pick_ref, maps_ref, packed_ref):
    count = packed_ref.shape[0]
    base = pl.program_id(0) * count
    for k in range(count):
        pick = pick_ref[base + k]
        col = pl.multiple_of((pick % 2) * TILE, TILE)
        packed_ref[k] = maps_ref[pick // 2, :, pl.ds(col, TILE), :]


def pack_tiles(bev_maps, picks, per_step=8):
    vehicles, height, width_cells, channels = bev_maps.shape
    slots = picks.shape[0]
    return pl.pallas_call(
        pack_kernel,
        grid_spec=pltpu.PrefetchScalarGridSpec(
            num_scalar_prefetch=1,
            grid=(slots // per_step,),
            in_specs=[pl.BlockSpec(bev_maps.shape, lambda i, *_: (0, 0, 0, 0))],
            out_specs=pl.BlockSpec((per_step, height, TILE, channels), lambda i, *_: (i, 0, 0, 0)),
        ),
        out_shape=jax.ShapeDtypeStruct((slots, height, TILE, channels), bf16),
        compiler_params=pltpu.CompilerParams(dimension_semantics=("arbitrary",)),
        name="pack_tiles",
    )(picks, bev_maps)


def row_halo(cells):
    count = lax.axis_size("row")
    height = cells.shape[1]
    return (
        lax.ppermute(cells[:, height - 1 :], "row", [(i, i + 1) for i in range(count - 1)]),
        lax.ppermute(cells[:, :1], "row", [(i + 1, i) for i in range(count - 1)]),
    )


def on_device(bev_maps, senders, shifts, counts, agent_query, agent_keyvalue, agent_out, agent_scale,
              conv_weight, gain_first, window_in, window_out, window_scale, gain_second, hidden_up,
              hidden_down):
    vehicles_here, height, width_cells, channels = bev_maps.shape
    agents = senders.shape[1]
    devices = lax.axis_size("veh")
    myself = lax.axis_index("veh")
    tile_cols = width_cells // TILE
    pair_count = vehicles_here * agents
    capacity = 2
    send_all = senders.reshape(devices, pair_count)
    shift_all = shifts.reshape(devices, pair_count)
    live_all = (jnp.arange(agents)[None, :] < counts[:, None]).reshape(devices, pair_count)
    tiles_all = jnp.where(live_all, tile_cols - jnp.abs(shift_all), 0)
    source_all = send_all // vehicles_here
    outgoing = jnp.where(source_all == myself, tiles_all, 0)
    before = (jnp.arange(pair_count)[:, None] < jnp.arange(pair_count)[None, :]).astype(f32)
    slot_start = jnp.dot(outgoing.astype(f32), before).astype(jnp.int32)
    base = (send_all % vehicles_here) * tile_cols + jnp.maximum(shift_all, 0)
    slot = jnp.arange(capacity)[None, :, None]
    step = slot - slot_start[:, None, :]
    hit = (step >= 0) & (step < outgoing[:, None, :])
    picks = jnp.sum(jnp.where(hit, base[:, None, :] + step, 0), axis=2).reshape(-1)
    packed = pack_tiles(bev_maps, picks).reshape(devices, capacity, height, TILE, channels)
    arrived = lax.all_to_all(packed, "veh", split_axis=0, concat_axis=0, tiled=True)
    arrived = arrived.reshape(devices * capacity, height, TILE, channels)

    tile_step = jnp.arange(tile_cols, dtype=jnp.int32)
    my_sources = source_all[myself]
    my_shifts = shift_all[myself]
    my_tiles = tiles_all[myself]
    earlier = (my_sources[None, :] == my_sources[:, None]) & (before.T > 0)
    offset = jnp.sum(jnp.where(earlier, my_tiles[None, :], 0), axis=1)
    shifted = tile_step[None, :] + my_shifts[:, None]
    inside = (shifted >= 0) & (shifted < tile_cols) & live_all[myself][:, None]
    slots = (
        my_sources[:, None] * capacity
        + offset[:, None]
        + tile_step[None, :]
        - jnp.maximum(-my_shifts, 0)[:, None]
    )
    slots = jnp.where(inside, slots, 0)
    per_tile = lambda x: x.reshape(vehicles_here, agents, tile_cols).transpose(0, 2, 1).reshape(-1, agents)
    bev_halo = row_halo(bev_maps)
    joined = agent_stage(bev_maps, arrived, per_tile(slots), per_tile(inside.astype(jnp.int32)),
                         agent_query, agent_keyvalue, agent_out, agent_scale)
    joined_halo = row_halo(joined)
    return layer_stage(bev_maps, joined, bev_halo, joined_halo, conv_weight, gain_first, window_in,
                       window_out, window_scale, gain_second, hidden_up, hidden_down)


def solution(mesh):
    split = P("veh", "row", None, None)
    return jax.shard_map(
        on_device, mesh=mesh, in_specs=(split,) + (P(),) * 15, out_specs=split, check_vma=False
    )
```

```python
import functools
import jax
import jax.numpy as jnp
from jax import lax
from jax.experimental import pallas as pl
from jax.experimental.pallas import tpu as pltpu
from jax.sharding import PartitionSpec as P

TILE = 32
WIN = 8
HEAD = 32
norm_eps = 1e-05
unit_eps = 1e-06
f32 = jnp.float32
bf16 = jnp.bfloat16


def nt_dot(a, b):
    return lax.dot_general(a, b, (((1,), (1,)), ((), ())), preferred_element_type=f32)


def halves(x):
    high = x.astype(bf16)
    return high, (x - high.astype(f32)).astype(bf16)


def head_sums(x, member):
    return jnp.dot(jnp.concatenate(halves(x), axis=-1), member, preferred_element_type=f32)


def agent_kernel(slot_ref, live_ref, ego_ref, t0, t1, t2, t3, query_ref, keyvalue_ref, out_w_ref,
                 scale_ref, member_ref, joined_ref):
    step = pl.program_id(0)
    tiles = (t0, t1, t2, t3)
    height, cols, channels = ego_ref.shape[1:]
    cells = height * cols
    ego = ego_ref[0].reshape(cells, channels)
    member = member_ref[...]
    query = jnp.dot(ego, query_ref[...], preferred_element_type=f32)
    query = query * (lax.rsqrt(head_sums(query * query, member) + unit_eps) * scale_ref[...])
    scores, values = [], []
    for a in range(len(tiles) + 1):
        source = ego if a == 0 else tiles[a - 1][0].reshape(cells, channels)
        keyvalue = jnp.dot(source, keyvalue_ref[...], preferred_element_type=f32).astype(bf16)
        key = keyvalue[:, :channels].astype(f32)
        values.append(keyvalue[:, channels:])
        score = head_sums(query * key, member) * lax.rsqrt(head_sums(key * key, member) + unit_eps)
        if a:
            score = score + jnp.where(live_ref[step * len(tiles) + a - 1] > 0, 0.0, -1e30)
        scores.append(score)
    top = functools.reduce(jnp.maximum, scores)
    total, mix = None, None
    for score, value in zip(scores, values):
        weight = jnp.exp(score - top)
        total = weight if total is None else total + weight
        part = weight * value.astype(f32)
        mix = part if mix is None else mix + part
    mix = (mix / total).astype(bf16)
    joined = jnp.dot(mix, out_w_ref[...], preferred_element_type=f32).astype(bf16)
    joined_ref[0] = joined.reshape(height, cols, channels)


def member_matrix(width):
    rows = jnp.arange(2 * width)[:, None] % width // HEAD
    return (rows == jnp.arange(width)[None, :] // HEAD).astype(bf16)


def agent_stage(bev_maps, arrived, slots, live, agent_query, agent_keyvalue, agent_out, agent_scale):
    vehicles, height, width_cells, channels = bev_maps.shape
    tile_cols = width_cells // TILE
    agents = slots.shape[1]
    full = lambda i, *_: (0, 0)
    ego_spec = pl.BlockSpec((1, height, TILE, channels), lambda i, *_: (i // tile_cols, 0, i % tile_cols, 0))
    tile_specs = [
        pl.BlockSpec((1, height, TILE, channels), lambda i, s, l, a=a: (s[i * agents + a], 0, 0, 0))
        for a in range(agents)
    ]
    scale_row = jnp.repeat(agent_scale, channels // agent_scale.shape[0])[None]
    return pl.pallas_call(
        agent_kernel,
        grid_spec=pltpu.PrefetchScalarGridSpec(
            num_scalar_prefetch=2,
            grid=(vehicles * tile_cols,),
            in_specs=[ego_spec, *tile_specs]
            + [pl.BlockSpec(w.shape, full) for w in (agent_query, agent_keyvalue, agent_out)]
            + [pl.BlockSpec((1, channels), full), pl.BlockSpec((2 * channels, channels), full)],
            out_specs=ego_spec,
        ),
        out_shape=jax.ShapeDtypeStruct(bev_maps.shape, bf16),
        compiler_params=pltpu.CompilerParams(dimension_semantics=("arbitrary",)),
        name="agent_stage",
    )(slots.reshape(-1), live.reshape(-1), bev_maps, arrived, arrived, arrived, arrived, agent_query,
      agent_keyvalue, agent_out, scale_row, member_matrix(channels))


def layer_norm(x, gain):
    centred = x - jnp.mean(x, axis=-1, keepdims=True)
    spread = jnp.mean(centred * centred, axis=-1, keepdims=True)
    return (centred * lax.rsqrt(spread + norm_eps) * gain).astype(bf16)


def layer_kernel(bev_ref, joined_ref, bev_up, bev_down, joined_up, joined_down, conv_ref, gain1_ref,
                 in_ref, out_w_ref, scale_ref, gain2_ref, up_ref, down_ref, member_ref, out_ref,
                 mixed_ref, attended_ref):
    height, cols, channels = bev_ref.shape[1:]
    cells = height * cols
    windows = cols // WIN
    area = WIN * WIN
    width = 2 * channels
    column = lax.broadcasted_iota(jnp.int32, (cells, channels), 0) % cols
    for half, (main, top, bottom) in enumerate(
        ((bev_ref, bev_up, bev_down), (joined_ref, joined_up, joined_down))
    ):
        lanes = slice(half * channels, (half + 1) * channels)
        rows = jnp.concatenate([top[0], main[0], bottom[0]], axis=0).astype(f32)
        sums = []
        for dj in range(3):
            taps = [conv_ref[di * 3 + dj : di * 3 + dj + 1, lanes] for di in range(3)]
            if dj == 1:
                taps[1] = taps[1] + 1.0
            acc = rows[0:height] * taps[0] + rows[1 : height + 1] * taps[1] + rows[2:] * taps[2]
            sums.append(acc.reshape(cells, channels))
        mixed = (
            sums[1]
            + jnp.where(column == 0, 0.0, pltpu.roll(sums[0], 1, axis=0))
            + jnp.where(column == cols - 1, 0.0, pltpu.roll(sums[2], cells - 1, axis=0))
        )
        for r in range(height):
            for w in range(windows):
                mixed_ref[w * area + r * WIN : w * area + (r + 1) * WIN, lanes] = mixed[
                    r * cols + w * WIN : r * cols + (w + 1) * WIN
                ]
    mixed = mixed_ref[...]
    hidden = layer_norm(mixed, gain1_ref[...])
    projected = jnp.dot(hidden, in_ref[...], preferred_element_type=f32)
    member = member_ref[...]
    groups = []
    for g in range(width // channels):
        lanes = slice(g * channels, (g + 1) * channels)
        query = projected[:, g * channels : (g + 1) * channels]
        key = projected[:, width + g * channels : width + (g + 1) * channels]
        query = query * (lax.rsqrt(head_sums(query * query, member) + unit_eps) * scale_ref[:, lanes])
        key = key * lax.rsqrt(head_sums(key * key, member) + unit_eps)
        value = projected[:, 2 * width + g * channels : 2 * width + (g + 1) * channels].astype(bf16)
        groups.append((jnp.concatenate(halves(query), axis=-1), *halves(key), value))
    heads = channels // HEAD
    head_of = lax.broadcasted_iota(jnp.int32, (area, 2 * channels), 1) % channels // HEAD
    lane_head = lax.broadcasted_iota(jnp.int32, (area, channels), 1) // HEAD
    for w in range(windows):
        span = slice(w * area, (w + 1) * area)
        for g, (query, key_high, key_low, value) in enumerate(groups):
            q = query[span]
            spread_q = jnp.concatenate(
                [jnp.where(head_of == j, q, jnp.zeros_like(q)) for j in range(heads)], axis=0
            )
            kh = key_high[span]
            scores = nt_dot(jnp.concatenate([kh, kh], axis=-1), spread_q) + nt_dot(
                key_low[span], spread_q[:, :channels]
            )
            weight = jnp.exp(scores - jnp.max(scores, axis=0, keepdims=True))
            weight = weight * (1.0 / jnp.sum(weight, axis=0, keepdims=True))
            mixed_values = jnp.dot(weight.T.astype(bf16), value[span], preferred_element_type=f32)
            attended = jnp.where(lane_head == 0, mixed_values[:area], 0.0)
            for j in range(1, heads):
                attended = jnp.where(lane_head == j, mixed_values[j * area : (j + 1) * area], attended)
            attended_ref[span, g * channels : (g + 1) * channels] = attended.astype(bf16)
    mixed = mixed + jnp.dot(attended_ref[...], out_w_ref[...], preferred_element_type=f32)
    hidden = layer_norm(mixed, gain2_ref[...])
    inner = jnp.dot(hidden, up_ref[...], preferred_element_type=f32)
    inner = (inner / (1.0 + jnp.exp(-inner))).astype(bf16)
    result = mixed + jnp.dot(inner, down_ref[...], preferred_element_type=f32)
    for r in range(height):
        for w in range(0, windows, 2):
            pair = [result[v * area + r * WIN : v * area + (r + 1) * WIN] for v in (w, w + 1)]
            out_ref[0, r, w * WIN : (w + 2) * WIN, :] = jnp.concatenate(pair, axis=0).astype(bf16)


def layer_stage(bev_maps, joined, bev_halo, joined_halo, conv_weight, gain_first, window_in, window_out,
                window_scale, gain_second, hidden_up, hidden_down):
    vehicles, height, width_cells, channels = bev_maps.shape
    width = 2 * channels
    cells = height * width_cells
    block = pl.BlockSpec((1, height, width_cells, channels), lambda i: (i, 0, 0, 0))
    edge = pl.BlockSpec((1, 1, width_cells, channels), lambda i: (i, 0, 0, 0))
    small = (
        conv_weight.reshape(9, width),
        gain_first[None],
        window_in,
        window_out,
        jnp.repeat(window_scale, width // window_scale.shape[0])[None],
        gain_second[None],
        hidden_up,
        hidden_down,
        member_matrix(channels),
    )
    return pl.pallas_call(
        layer_kernel,
        grid=(vehicles,),
        in_specs=[block, block, edge, edge, edge, edge]
        + [pl.BlockSpec(w.shape, lambda i: (0, 0)) for w in small],
        out_specs=pl.BlockSpec((1, height, width_cells, width), lambda i: (i, 0, 0, 0)),
        out_shape=jax.ShapeDtypeStruct((vehicles, height, width_cells, width), bf16),
        scratch_shapes=[pltpu.VMEM((cells, width), f32), pltpu.VMEM((cells, width), bf16)],
        compiler_params=pltpu.CompilerParams(dimension_semantics=("arbitrary",)),
        name="layer_stage",
    )(bev_maps, joined, *bev_halo, *joined_halo, *small)


RING = 8
PLANE = 8
HOPS = (0, -1, 1, -2, 2, -3, 3, 4)
PIECES = 4
SLOTS = 2


def exchange_kernel(vehicle_ref, tile_ref, maps_ref, arrived_ref, f1, f2, f3, b1, b2, b3, far, outbox, ring_send,
                    ring_recv, plane_send, plane_recv, own_sem):
    me = lax.axis_index("veh")
    plane, seat = me // PLANE, me % PLANE
    depth = maps_ref.shape[0] // PIECES
    ahead = {"veh": lax.rem(plane + 1, RING) * PLANE + seat}
    behind = {"veh": lax.rem(plane + RING - 1, RING) * PLANE + seat}
    peers = [{"veh": plane * PLANE + lax.rem(seat + j, PLANE)} for j in range(PLANE)]

    barrier = pltpu.get_barrier_semaphore()
    for peer in (ahead, behind, *peers[1:]):
        pl.semaphore_signal(barrier, inc=1, device_id=peer, device_id_type=pl.DeviceIdType.MESH)
    pl.semaphore_wait(barrier, PLANE + 1)

    blocks = (maps_ref, f1, b1, f2, b2, f3, b3, far)
    started = []

    def pass_on(source, block, piece, target):
        span = pl.ds(piece * depth, depth)
        copy = pltpu.make_async_remote_copy(
            src_ref=blocks[source].at[span],
            dst_ref=blocks[block].at[span],
            send_sem=ring_send.at[block - 1, piece],
            recv_sem=ring_recv.at[block - 1, piece],
            device_id=target,
            device_id_type=pl.DeviceIdType.MESH,
        )
        copy.start()
        started.append(copy)

    def arrival(block, piece):
        span = pl.ds(piece * depth, depth)
        ref = blocks[block].at[span]
        pltpu.make_async_copy(ref, ref, ring_recv.at[block - 1, piece]).wait()

    def hand_out(block):
        held = blocks[block]

        def fill(j, carry):
            for slot in range(SLOTS):
                at = (block * PLANE + j) * SLOTS + slot
                outbox[block, j, slot] = held[vehicle_ref[at], :, tile_ref[at]]
            return carry

        lax.fori_loop(0, PLANE, fill, 0)
        for j in range(1, PLANE):
            pltpu.make_async_remote_copy(
                src_ref=outbox.at[block, j],
                dst_ref=arrived_ref.at[block, seat],
                send_sem=plane_send.at[0],
                recv_sem=plane_recv.at[0],
                device_id=peers[j],
                device_id_type=pl.DeviceIdType.MESH,
            ).start()
        pltpu.make_async_copy(outbox.at[block, 0], arrived_ref.at[block, seat], own_sem.at[block]).start()

    for piece in range(PIECES):
        pass_on(0, 1, piece, ahead)
        pass_on(0, 2, piece, behind)
    hand_out(0)
    for step in range(1, RING // 2):
        front, back = 2 * step - 1, 2 * step
        for piece in range(PIECES):
            arrival(front, piece)
            if step < RING // 2 - 1:
                pass_on(front, front + 2, piece, ahead)
            elif piece < PIECES // 2:
                pass_on(front, RING - 1, piece, ahead)
            arrival(back, piece)
            if step < RING // 2 - 1:
                pass_on(back, back + 2, piece, behind)
            elif piece >= PIECES // 2:
                pass_on(back, RING - 1, piece, behind)
        hand_out(front)
        hand_out(back)
    for piece in range(PIECES):
        arrival(RING - 1, piece)
    hand_out(RING - 1)
    for copy in started:
        copy.wait_send()
    sent = outbox.at[pl.ds(0, PLANE - 1)]
    pltpu.make_async_copy(sent, sent, plane_send.at[0]).wait()
    got = arrived_ref.at[pl.ds(0, PLANE - 1)]
    pltpu.make_async_copy(got, got, plane_recv.at[0]).wait()
    for block in range(RING):
        pltpu.make_async_copy(outbox.at[block, 0], arrived_ref.at[block, seat], own_sem.at[block]).wait()


def exchange(bev_maps, picks):
    vehicles, height, width_cells, channels = bev_maps.shape
    tile_cols = width_cells // TILE
    tiled = bev_maps.reshape(vehicles, height, tile_cols, TILE, channels)
    box = (RING, PLANE, SLOTS, height, TILE, channels)
    return pl.pallas_call(
        exchange_kernel,
        in_specs=[pl.BlockSpec(memory_space=pltpu.SMEM)] * 2 + [pl.BlockSpec(memory_space=pltpu.VMEM)],
        out_specs=pl.BlockSpec(memory_space=pl.ANY),
        out_shape=jax.ShapeDtypeStruct(box, bf16),
        scratch_shapes=[pltpu.VMEM(tiled.shape, bf16)] * (RING - 1)
        + [
            pltpu.VMEM(box, bf16),
            pltpu.SemaphoreType.DMA((RING - 1, PIECES)),
            pltpu.SemaphoreType.DMA((RING - 1, PIECES)),
            pltpu.SemaphoreType.DMA((1,)),
            pltpu.SemaphoreType.DMA((1,)),
            pltpu.SemaphoreType.DMA((RING,)),
        ],
        compiler_params=pltpu.CompilerParams(collective_id=0, has_side_effects=True),
        name="exchange",
    )(picks // tile_cols, picks % tile_cols, tiled)


def row_halo(cells):
    count = lax.axis_size("row")
    height = cells.shape[1]
    return (
        lax.ppermute(cells[:, height - 1 :], "row", [(i, i + 1) for i in range(count - 1)]),
        lax.ppermute(cells[:, :1], "row", [(i + 1, i) for i in range(count - 1)]),
    )


def route(senders, shifts, counts, vehicles_here, tile_cols):
    agents = senders.shape[1]
    devices = lax.axis_size("veh")
    myself = lax.axis_index("veh")
    plane, seat = myself // PLANE, myself % PLANE
    pair_count = vehicles_here * agents
    by_block = lambda x: lax.dynamic_slice_in_dim(x.reshape(devices, -1), plane * PLANE, PLANE, axis=0)
    sender = by_block(senders)
    shift = by_block(shifts)
    live = jnp.arange(agents)[None, None, :] < by_block(counts)[:, :, None]
    live = live.reshape(PLANE, pair_count)
    tiles = jnp.where(live, tile_cols - jnp.abs(shift), 0)
    source = sender // vehicles_here
    ordinal = jnp.arange(pair_count)
    earlier = ordinal[None, :, None] > ordinal[None, None, :]
    same = source[:, :, None] == source[:, None, :]
    start = jnp.sum(jnp.where(same & earlier, tiles[:, None, :], 0), axis=2)
    base = (sender % vehicles_here) * tile_cols + jnp.maximum(shift, 0)

    hops = jnp.asarray(HOPS, jnp.int32)
    origin = (plane + hops + RING) % RING * PLANE + seat
    order = (seat + jnp.arange(PLANE)) % PLANE
    turn = (order[:, None] == jnp.arange(PLANE)[None, :]).astype(jnp.int32)
    slot = jnp.arange(SLOTS)[None, None, :, None]
    step = slot - start[None, :, None, :]
    hit = (source[None, :, None, :] == origin[:, None, None, None]) & (step >= 0)
    hit = hit & (step < tiles[None, :, None, :])
    picks = jnp.sum(jnp.where(hit, base[None, :, None, :] + step, 0), axis=3)
    picks = jnp.sum(turn[None, :, :, None] * picks[:, None, :, :], axis=2).reshape(-1)

    mine = lambda x: lax.dynamic_index_in_dim(x, seat, axis=0, keepdims=False)
    my_source, my_shift, my_start, my_live = mine(source), mine(shift), mine(start), mine(live)
    away = (my_source // PLANE - plane + RING) % RING
    rank = jnp.where(away > RING // 2, 2 * (RING - away) - 1, jnp.maximum(2 * away, 0))
    rank = jnp.where(away == RING // 2, RING - 1, rank)
    tile_step = jnp.arange(tile_cols, dtype=jnp.int32)
    shifted = tile_step[None, :] + my_shift[:, None]
    inside = (shifted >= 0) & (shifted < tile_cols) & my_live[:, None]
    slots = ((rank * PLANE + my_source % PLANE) * SLOTS + my_start)[:, None] + tile_step[None, :]
    slots = slots - jnp.maximum(-my_shift, 0)[:, None]
    slots = jnp.where(inside, slots, 0)
    per_tile = lambda x: x.reshape(vehicles_here, agents, tile_cols).transpose(0, 2, 1).reshape(-1, agents)
    return picks, per_tile(slots), per_tile(inside.astype(jnp.int32))


def on_device(bev_maps, senders, shifts, counts, agent_query, agent_keyvalue, agent_out, agent_scale,
              conv_weight, gain_first, window_in, window_out, window_scale, gain_second, hidden_up,
              hidden_down):
    vehicles_here, height, width_cells, channels = bev_maps.shape
    picks, slots, live = route(senders, shifts, counts, vehicles_here, width_cells // TILE)
    arrived = exchange(bev_maps, picks).reshape(-1, height, TILE, channels)
    bev_halo = row_halo(bev_maps)
    joined = agent_stage(bev_maps, arrived, slots, live, agent_query, agent_keyvalue, agent_out,
                         agent_scale)
    joined_halo = row_halo(joined)
    return layer_stage(bev_maps, joined, bev_halo, joined_halo, conv_weight, gain_first, window_in,
                       window_out, window_scale, gain_second, hidden_up, hidden_down)


def solution(mesh):
    split = P("veh", "row", None, None)
    return jax.shard_map(
        on_device, mesh=mesh, in_specs=(split,) + (P(),) * 15, out_specs=split, check_vma=False
    )
```

```python
import functools
import jax
import jax.numpy as jnp
from jax import lax
from jax.experimental import pallas as pl
from jax.experimental.pallas import tpu as pltpu
from jax.sharding import PartitionSpec as P

TILE = 32
WIN = 8
HEAD = 32
norm_eps = 1e-05
unit_eps = 1e-06
f32 = jnp.float32
bf16 = jnp.bfloat16


def nt_dot(a, b):
    return lax.dot_general(a, b, (((1,), (1,)), ((), ())), preferred_element_type=f32)


def halves(x):
    high = x.astype(bf16)
    return high, (x - high.astype(f32)).astype(bf16)


def head_sums(x, member):
    return jnp.dot(jnp.concatenate(halves(x), axis=-1), member, preferred_element_type=f32)


def agent_kernel(slot_ref, live_ref, ego_ref, t0, t1, t2, t3, query_ref, keyvalue_ref, out_w_ref,
                 scale_ref, joined_ref):
    step = pl.program_id(0)
    tiles = (t0, t1, t2, t3)
    height, cols, channels = ego_ref.shape[1:]
    cells = height * cols
    ego = ego_ref[0].reshape(cells, channels)
    member = member_matrix(channels)
    query = jnp.dot(ego, query_ref[...], preferred_element_type=f32)
    count = len(tiles) + 1
    sources = jnp.concatenate([ego] + [t[0].reshape(cells, channels) for t in tiles], axis=0)
    keyvalue = jnp.dot(sources, keyvalue_ref[...], preferred_element_type=f32).astype(bf16)
    query = query * (lax.rsqrt(head_sums(query * query, member) + unit_eps) * scale_row(scale_ref, 0, channels))
    key = keyvalue[:, :channels].astype(f32)
    norms = head_sums(key * key, member)
    products = head_sums((key.reshape(count, cells, channels) * query[None]).reshape(count * cells, channels), member)
    score = products * lax.rsqrt(norms + unit_eps)
    scores = [score[a * cells : (a + 1) * cells] for a in range(count)]
    values = [keyvalue[a * cells : (a + 1) * cells, channels:] for a in range(count)]
    for a in range(len(tiles)):
        scores[a + 1] = scores[a + 1] + jnp.where(live_ref[step * len(tiles) + a] > 0, 0.0, -1e30)
    top = functools.reduce(jnp.maximum, scores)
    total, mix = None, None
    for score, value in zip(scores, values):
        weight = jnp.exp(score - top)
        total = weight if total is None else total + weight
        part = weight * value.astype(f32)
        mix = part if mix is None else mix + part
    mix = (mix / total).astype(bf16)
    joined = jnp.dot(mix, out_w_ref[...], preferred_element_type=f32).astype(bf16)
    joined_ref[0] = joined.reshape(height, cols, channels)


def member_matrix(width):
    rows = lax.broadcasted_iota(jnp.int32, (2 * width, width), 0) % width // HEAD
    lanes = lax.broadcasted_iota(jnp.int32, (2 * width, width), 1) // HEAD
    return jnp.where(rows == lanes, 1.0, 0.0).astype(bf16)


def scale_row(scale_ref, first, width):
    head = lax.broadcasted_iota(jnp.int32, (1, width), 1) // HEAD
    row = jnp.full((1, width), scale_ref[first], f32)
    for j in range(1, width // HEAD):
        row = jnp.where(head == j, scale_ref[first + j], row)
    return row


def agent_stage(bev_maps, arrived, slots, live, agent_query, agent_keyvalue, agent_out, agent_scale):
    vehicles, height, width_cells, channels = bev_maps.shape
    tile_cols = width_cells // TILE
    agents = slots.shape[1]
    full = lambda i, *_: (0, 0)
    ego_spec = pl.BlockSpec((1, height, TILE, channels), lambda i, *_: (i // tile_cols, 0, i % tile_cols, 0))
    tile_specs = [
        pl.BlockSpec((1, height, TILE, channels), lambda i, s, l, a=a: (s[i * agents + a], 0, 0, 0))
        for a in range(agents)
    ]
    return pl.pallas_call(
        agent_kernel,
        grid_spec=pltpu.PrefetchScalarGridSpec(
            num_scalar_prefetch=2,
            grid=(vehicles * tile_cols,),
            in_specs=[ego_spec, *tile_specs]
            + [pl.BlockSpec(w.shape, full) for w in (agent_query, agent_keyvalue, agent_out)]
            + [pl.BlockSpec(memory_space=pltpu.SMEM)],
            out_specs=ego_spec,
        ),
        out_shape=jax.ShapeDtypeStruct(bev_maps.shape, bf16),
        compiler_params=pltpu.CompilerParams(dimension_semantics=("arbitrary",)),
        name="agent_stage",
    )(slots.reshape(-1), live.reshape(-1), bev_maps, arrived, arrived, arrived, arrived, agent_query,
      agent_keyvalue, agent_out, agent_scale)


def layer_norm(x, gain):
    centred = x - jnp.mean(x, axis=-1, keepdims=True)
    spread = jnp.mean(centred * centred, axis=-1, keepdims=True)
    return (centred * lax.rsqrt(spread + norm_eps) * gain).astype(bf16)


def layer_kernel(bev_ref, joined_ref, bev_up, bev_down, joined_up, joined_down, conv_ref, gain1_ref,
                 in_ref, out_w_ref, scale_ref, gain2_ref, up_ref, down_ref, out_ref,
                 mixed_ref, attended_ref):
    height, cols, channels = bev_ref.shape[1:]
    cells = height * cols
    windows = cols // WIN
    area = WIN * WIN
    width = 2 * channels
    column = lax.broadcasted_iota(jnp.int32, (cells, channels), 0) % cols
    band = lax.axis_index("row")
    has_up = jnp.where(band > 0, 1.0, 0.0)
    has_down = jnp.where(band < lax.axis_size("row") - 1, 1.0, 0.0)
    for half, (main, top, bottom) in enumerate(
        ((bev_ref, bev_up, bev_down), (joined_ref, joined_up, joined_down))
    ):
        lanes = slice(half * channels, (half + 1) * channels)
        rows = jnp.concatenate(
            [top[0].astype(f32) * has_up, main[0].astype(f32), bottom[0].astype(f32) * has_down], axis=0
        )
        sums = []
        for dj in range(3):
            taps = [conv_ref[di, dj : dj + 1, lanes] for di in range(3)]
            if dj == 1:
                taps[1] = taps[1] + 1.0
            acc = rows[0:height] * taps[0] + rows[1 : height + 1] * taps[1] + rows[2:] * taps[2]
            sums.append(acc.reshape(cells, channels))
        mixed = (
            sums[1]
            + jnp.where(column == 0, 0.0, pltpu.roll(sums[0], 1, axis=0))
            + jnp.where(column == cols - 1, 0.0, pltpu.roll(sums[2], cells - 1, axis=0))
        )
        for r in range(height):
            for w in range(windows):
                mixed_ref[w * area + r * WIN : w * area + (r + 1) * WIN, lanes] = mixed[
                    r * cols + w * WIN : r * cols + (w + 1) * WIN
                ]
    mixed = mixed_ref[...]
    hidden = layer_norm(mixed, gain1_ref[...])
    projected = jnp.dot(hidden, in_ref[...], preferred_element_type=f32)
    member = member_matrix(channels)
    groups = []
    for g in range(width // channels):
        query = projected[:, g * channels : (g + 1) * channels]
        key = projected[:, width + g * channels : width + (g + 1) * channels]
        query = query * (lax.rsqrt(head_sums(query * query, member) + unit_eps) * scale_row(scale_ref, g * (channels // HEAD), channels))
        key = key * lax.rsqrt(head_sums(key * key, member) + unit_eps)
        value = projected[:, 2 * width + g * channels : 2 * width + (g + 1) * channels].astype(bf16)
        groups.append((jnp.concatenate(halves(query), axis=-1), *halves(key), value))
    heads = channels // HEAD
    head_of = lax.broadcasted_iota(jnp.int32, (area, 2 * channels), 1) % channels // HEAD
    lane_head = lax.broadcasted_iota(jnp.int32, (area, channels), 1) // HEAD
    def score_of(w, g):
        query, key_high, key_low, value = groups[g]
        span = slice(w * area, (w + 1) * area)
        q = query[span]
        spread_q = jnp.concatenate(
            [jnp.where(head_of == j, q, jnp.zeros_like(q)) for j in range(heads)], axis=0
        )
        kh = key_high[span]
        return nt_dot(jnp.concatenate([kh, kh], axis=-1), spread_q) + nt_dot(
            key_low[span], spread_q[:, :channels]
        )

    def soften(scores):
        weight = jnp.exp(scores - jnp.max(scores, axis=0, keepdims=True))
        return (weight * (1.0 / jnp.sum(weight, axis=0, keepdims=True))).astype(bf16)

    def finish(w, g, weight):
        span = slice(w * area, (w + 1) * area)
        mixed_values = lax.dot_general(weight, groups[g][3][span], (((0,), (0,)), ((), ())), preferred_element_type=f32)
        attended = mixed_values[:area]
        for j in range(1, heads):
            attended = jnp.where(lane_head == j, mixed_values[j * area : (j + 1) * area], attended)
        attended_ref[span, g * channels : (g + 1) * channels] = attended.astype(bf16)

    units = [(w, g) for w in range(windows) for g in range(len(groups))]
    all_scores = [score_of(w, g) for w, g in units]
    all_weights = [soften(s) for s in all_scores]
    for (w, g), weight in zip(units, all_weights):
        finish(w, g, weight)
    mixed = mixed + jnp.dot(attended_ref[...], out_w_ref[...], preferred_element_type=f32)
    hidden = layer_norm(mixed, gain2_ref[...])
    inner = jnp.dot(hidden, up_ref[...], preferred_element_type=f32)
    inner = (inner / (1.0 + jnp.exp(-inner))).astype(bf16)
    result = mixed + jnp.dot(inner, down_ref[...], preferred_element_type=f32)
    for r in range(height):
        for w in range(0, windows, 2):
            pair = [result[v * area + r * WIN : v * area + (r + 1) * WIN] for v in (w, w + 1)]
            out_ref[0, r, w * WIN : (w + 2) * WIN, :] = jnp.concatenate(pair, axis=0).astype(bf16)


def layer_stage(bev_maps, joined, bev_halo, joined_halo, conv_weight, gain_first, window_in, window_out,
                window_scale, gain_second, hidden_up, hidden_down):
    vehicles, height, width_cells, channels = bev_maps.shape
    width = 2 * channels
    cells = height * width_cells
    block = pl.BlockSpec((1, height, width_cells, channels), lambda i: (i, 0, 0, 0))
    edge = pl.BlockSpec((1, 1, width_cells, channels), lambda i: (i, 0, 0, 0))
    small = (conv_weight, gain_first[None], window_in, window_out, window_scale, gain_second[None],
             hidden_up, hidden_down)
    whole = lambda w: pl.BlockSpec(w.shape, lambda i: (0,) * w.ndim)
    scalars = pl.BlockSpec(memory_space=pltpu.SMEM)
    return pl.pallas_call(
        layer_kernel,
        grid=(vehicles,),
        in_specs=[block, block, edge, edge, edge, edge]
        + [scalars if w is window_scale else whole(w) for w in small],
        out_specs=pl.BlockSpec((1, height, width_cells, width), lambda i: (i, 0, 0, 0)),
        out_shape=jax.ShapeDtypeStruct((vehicles, height, width_cells, width), bf16),
        scratch_shapes=[pltpu.VMEM((cells, width), f32), pltpu.VMEM((cells, width), bf16)],
        compiler_params=pltpu.CompilerParams(dimension_semantics=("arbitrary",)),
        name="layer_stage",
    )(bev_maps, joined, *bev_halo, *joined_halo, *small)


RING = 8
PLANE = 8
HOPS = (0, -1, 1, -2, 2, -3, 3, 4)
PIECES = 2
SLOTS = 2


def exchange_kernel(vehicle_ref, tile_ref, maps_ref, arrived_ref, up_ref, down_ref, *scratch):
    outbox, ring_send, ring_recv, plane_send, plane_recv, own_sem, edge_send, edge_recv = scratch[-8:]
    me = lax.axis_index("veh")
    plane, seat = me // PLANE, me % PLANE
    height = maps_ref.shape[1]
    bands = lax.axis_size("row")
    band = lax.axis_index("row")
    below = {"row": lax.rem(band + 1, bands)}
    above = {"row": lax.rem(band + bands - 1, bands)}
    ahead = {"veh": lax.rem(plane + 1, RING) * PLANE + seat}
    behind = {"veh": lax.rem(plane + RING - 1, RING) * PLANE + seat}
    peers = [{"veh": plane * PLANE + lax.rem(seat + j, PLANE)} for j in range(PLANE)]

    barrier = pltpu.get_barrier_semaphore()
    for peer in (ahead, behind, below, above, *peers[1:]):
        pl.semaphore_signal(barrier, inc=1, device_id=peer, device_id_type=pl.DeviceIdType.MESH)
    pl.semaphore_wait(barrier, PLANE + 3)

    started = []

    def held(block, piece):
        if block == 0:
            return maps_ref.at[:, :, :, piece]
        return scratch[(block - 1) * PIECES + piece]

    def pass_on(source, block, piece, target):
        copy = pltpu.make_async_remote_copy(
            src_ref=held(source, piece),
            dst_ref=held(block, piece),
            send_sem=ring_send.at[block - 1, piece],
            recv_sem=ring_recv.at[block - 1, piece],
            device_id=target,
            device_id_type=pl.DeviceIdType.MESH,
        )
        copy.start()
        started.append(copy)

    def arrival(block, piece):
        ref = held(block, piece)
        pltpu.make_async_copy(ref, ref, ring_recv.at[block - 1, piece]).wait()

    def hand_out(block, piece):
        source = held(block, piece)

        def fill(j, carry):
            for slot in range(SLOTS):
                at = (block * PLANE + j) * SLOTS + slot
                outbox[block, j, slot, :, piece] = source[vehicle_ref[at], :, tile_ref[at]]
            return carry

        lax.fori_loop(0, PLANE, fill, 0)
        for j in range(1, PLANE):
            pltpu.make_async_remote_copy(
                src_ref=outbox.at[block, j, :, :, piece],
                dst_ref=arrived_ref.at[block, seat, :, :, piece],
                send_sem=plane_send.at[0],
                recv_sem=plane_recv.at[0],
                device_id=peers[j],
                device_id_type=pl.DeviceIdType.MESH,
            ).start()

    edges = []
    for at, (row, ref, target) in enumerate(((height - 1, up_ref, below), (0, down_ref, above))):
        edge = pltpu.make_async_remote_copy(
            src_ref=maps_ref.at[:, row],
            dst_ref=ref,
            send_sem=edge_send.at[at],
            recv_sem=edge_recv.at[at],
            device_id=target,
            device_id_type=pl.DeviceIdType.MESH,
        )
        edge.start()
        edges.append(edge)
    for piece in range(PIECES):
        pass_on(0, 1, piece, ahead)
        pass_on(0, 2, piece, behind)
    for piece in range(PIECES):
        hand_out(0, piece)
    for step in range(1, RING // 2):
        front, back = 2 * step - 1, 2 * step
        for piece in range(PIECES):
            arrival(front, piece)
            if step < RING // 2 - 1:
                pass_on(front, front + 2, piece, ahead)
            elif piece < PIECES // 2:
                pass_on(front, RING - 1, piece, ahead)
            arrival(back, piece)
            if step < RING // 2 - 1:
                pass_on(back, back + 2, piece, behind)
            elif piece >= PIECES // 2:
                pass_on(back, RING - 1, piece, behind)
            hand_out(front, piece)
            hand_out(back, piece)
    for piece in range(PIECES):
        arrival(RING - 1, piece)
        hand_out(RING - 1, piece)
    for block in range(RING):
        pltpu.make_async_copy(outbox.at[block, 0], arrived_ref.at[block, seat], own_sem.at[block]).start()
    for edge in edges:
        edge.wait()
    for copy in started:
        copy.wait_send()
    sent = outbox.at[pl.ds(0, PLANE - 1)]
    pltpu.make_async_copy(sent, sent, plane_send.at[0]).wait()
    got = arrived_ref.at[pl.ds(0, PLANE - 1)]
    pltpu.make_async_copy(got, got, plane_recv.at[0]).wait()
    for block in range(RING):
        pltpu.make_async_copy(outbox.at[block, 0], arrived_ref.at[block, seat], own_sem.at[block]).wait()


def exchange(bev_maps, picks):
    vehicles, height, width_cells, channels = bev_maps.shape
    tile_cols = width_cells // TILE
    part = TILE // PIECES
    tiled = bev_maps.reshape(vehicles, height, tile_cols, PIECES, part, channels)
    box = (RING, PLANE, SLOTS, height, PIECES, part, channels)
    edge = (vehicles,) + tiled.shape[2:]
    shapes = (box, edge, edge)
    arrived, up, down = pl.pallas_call(
        exchange_kernel,
        in_specs=[pl.BlockSpec(memory_space=pltpu.SMEM)] * 2 + [pl.BlockSpec(memory_space=pltpu.VMEM)],
        out_specs=[pl.BlockSpec(memory_space=pl.ANY)] * 3,
        out_shape=[jax.ShapeDtypeStruct(s, bf16) for s in shapes],
        scratch_shapes=[pltpu.VMEM(tiled.shape[:3] + tiled.shape[4:], bf16)] * ((RING - 1) * PIECES)
        + [
            pltpu.VMEM(box, bf16),
            pltpu.SemaphoreType.DMA((RING - 1, PIECES)),
            pltpu.SemaphoreType.DMA((RING - 1, PIECES)),
            pltpu.SemaphoreType.DMA((1,)),
            pltpu.SemaphoreType.DMA((1,)),
            pltpu.SemaphoreType.DMA((RING,)),
            pltpu.SemaphoreType.DMA((2,)),
            pltpu.SemaphoreType.DMA((2,)),
        ],
        compiler_params=pltpu.CompilerParams(collective_id=0, has_side_effects=True),
        name="exchange",
    )(picks // tile_cols, picks % tile_cols, tiled)
    flat = (vehicles, 1, width_cells, channels)
    return arrived.reshape(-1, height, TILE, channels), (up.reshape(flat), down.reshape(flat))


def row_halo(cells):
    count = lax.axis_size("row")
    height = cells.shape[1]
    return (
        lax.ppermute(cells[:, height - 1 :], "row", [(i, i + 1) for i in range(count - 1)]),
        lax.ppermute(cells[:, :1], "row", [(i + 1, i) for i in range(count - 1)]),
    )


def route(senders, shifts, counts, vehicles_here, tile_cols):
    agents = senders.shape[1]
    devices = lax.axis_size("veh")
    myself = lax.axis_index("veh")
    plane, seat = myself // PLANE, myself % PLANE
    pair_count = vehicles_here * agents
    by_block = lambda x: lax.dynamic_slice_in_dim(x.reshape(devices, -1), plane * PLANE, PLANE, axis=0)
    sender = by_block(senders)
    shift = by_block(shifts)
    live = jnp.arange(agents)[None, None, :] < by_block(counts)[:, :, None]
    live = live.reshape(PLANE, pair_count)
    tiles = jnp.where(live, tile_cols - jnp.abs(shift), 0)
    source = sender // vehicles_here
    ordinal = jnp.arange(pair_count)
    earlier = ordinal[None, :, None] > ordinal[None, None, :]
    same = source[:, :, None] == source[:, None, :]
    start = jnp.sum(jnp.where(same & earlier, tiles[:, None, :], 0), axis=2)
    base = (sender % vehicles_here) * tile_cols + jnp.maximum(shift, 0)

    hops = jnp.asarray(HOPS, jnp.int32)
    origin = (plane + hops + RING) % RING * PLANE + seat
    order = (seat + jnp.arange(PLANE)) % PLANE
    turn = (order[:, None] == jnp.arange(PLANE)[None, :]).astype(jnp.int32)
    slot = jnp.arange(SLOTS)[None, None, :, None]
    step = slot - start[None, :, None, :]
    hit = (source[None, :, None, :] == origin[:, None, None, None]) & (step >= 0)
    hit = hit & (step < tiles[None, :, None, :])
    picks = jnp.sum(jnp.where(hit, base[None, :, None, :] + step, 0), axis=3)
    picks = jnp.sum(turn[None, :, :, None] * picks[:, None, :, :], axis=2).reshape(-1)

    mine = lambda x: lax.dynamic_index_in_dim(x, seat, axis=0, keepdims=False)
    my_source, my_shift, my_start, my_live = mine(source), mine(shift), mine(start), mine(live)
    away = (my_source // PLANE - plane + RING) % RING
    rank = jnp.where(away > RING // 2, 2 * (RING - away) - 1, jnp.maximum(2 * away, 0))
    rank = jnp.where(away == RING // 2, RING - 1, rank)
    tile_step = jnp.arange(tile_cols, dtype=jnp.int32)
    shifted = tile_step[None, :] + my_shift[:, None]
    inside = (shifted >= 0) & (shifted < tile_cols) & my_live[:, None]
    slots = ((rank * PLANE + my_source % PLANE) * SLOTS + my_start)[:, None] + tile_step[None, :]
    slots = slots - jnp.maximum(-my_shift, 0)[:, None]
    slots = jnp.where(inside, slots, 0)
    per_tile = lambda x: x.reshape(vehicles_here, agents, tile_cols).transpose(0, 2, 1).reshape(-1, agents)
    return picks, per_tile(slots), per_tile(inside.astype(jnp.int32))


def on_device(bev_maps, senders, shifts, counts, agent_query, agent_keyvalue, agent_out, agent_scale,
              conv_weight, gain_first, window_in, window_out, window_scale, gain_second, hidden_up,
              hidden_down):
    vehicles_here, height, width_cells, channels = bev_maps.shape
    picks, slots, live = route(senders, shifts, counts, vehicles_here, width_cells // TILE)
    arrived, bev_halo = exchange(bev_maps, picks)
    joined = agent_stage(bev_maps, arrived, slots, live, agent_query, agent_keyvalue, agent_out,
                         agent_scale)
    joined_halo = row_halo(joined)
    return layer_stage(bev_maps, joined, bev_halo, joined_halo, conv_weight, gain_first, window_in,
                       window_out, window_scale, gain_second, hidden_up, hidden_down)


def solution(mesh):
    split = P("veh", "row", None, None)
    return jax.shard_map(
        on_device, mesh=mesh, in_specs=(split,) + (P(),) * 15, out_specs=split, check_vma=False
    )
```

```python
import functools
import jax
import jax.numpy as jnp
from jax import lax
from jax.experimental import pallas as pl
from jax.experimental.pallas import tpu as pltpu
from jax.sharding import PartitionSpec as P

TILE = 32
WIN = 8
HEAD = 32
norm_eps = 1e-05
unit_eps = 1e-06
f32 = jnp.float32
bf16 = jnp.bfloat16


def nt_dot(a, b):
    return lax.dot_general(a, b, (((1,), (1,)), ((), ())), preferred_element_type=f32)


def halves(x):
    high = x.astype(bf16)
    return high, (x - high.astype(f32)).astype(bf16)


def head_sums(x, member):
    return jnp.dot(jnp.concatenate(halves(x), axis=-1), member, preferred_element_type=f32)


def member_matrix(width):
    rows = lax.broadcasted_iota(jnp.int32, (2 * width, width), 0) % width // HEAD
    lanes = lax.broadcasted_iota(jnp.int32, (2 * width, width), 1) // HEAD
    return jnp.where(rows == lanes, 1.0, 0.0).astype(bf16)


def scale_row(scale_ref, first, width):
    head = lax.broadcasted_iota(jnp.int32, (1, width), 1) // HEAD
    row = jnp.full((1, width), scale_ref[first], f32)
    for j in range(1, width // HEAD):
        row = jnp.where(head == j, scale_ref[first + j], row)
    return row


def layer_norm(x, gain):
    centred = x - jnp.mean(x, axis=-1, keepdims=True)
    spread = jnp.mean(centred * centred, axis=-1, keepdims=True)
    return (centred * lax.rsqrt(spread + norm_eps) * gain).astype(bf16)


def layer_kernel(bev_ref, joined_ref, bev_up, bev_down, joined_up, joined_down, conv_ref, gain1_ref,
                 in_ref, out_w_ref, scale_ref, gain2_ref, up_ref, down_ref, out_ref,
                 mixed_ref, attended_ref):
    height, cols, channels = bev_ref.shape[1:]
    cells = height * cols
    windows = cols // WIN
    area = WIN * WIN
    width = 2 * channels
    column = lax.broadcasted_iota(jnp.int32, (cells, channels), 0) % cols
    band = lax.axis_index("row")
    has_up = jnp.where(band > 0, 1.0, 0.0)
    has_down = jnp.where(band < lax.axis_size("row") - 1, 1.0, 0.0)
    for half, (main, top, bottom) in enumerate(
        ((bev_ref, bev_up, bev_down), (joined_ref, joined_up, joined_down))
    ):
        lanes = slice(half * channels, (half + 1) * channels)
        rows = jnp.concatenate(
            [top[0].astype(f32) * has_up, main[0].astype(f32), bottom[0].astype(f32) * has_down], axis=0
        )
        sums = []
        for dj in range(3):
            taps = [conv_ref[di, dj : dj + 1, lanes] for di in range(3)]
            if dj == 1:
                taps[1] = taps[1] + 1.0
            acc = rows[0:height] * taps[0] + rows[1 : height + 1] * taps[1] + rows[2:] * taps[2]
            sums.append(acc.reshape(cells, channels))
        mixed = (
            sums[1]
            + jnp.where(column == 0, 0.0, pltpu.roll(sums[0], 1, axis=0))
            + jnp.where(column == cols - 1, 0.0, pltpu.roll(sums[2], cells - 1, axis=0))
        )
        for r in range(height):
            for w in range(windows):
                mixed_ref[w * area + r * WIN : w * area + (r + 1) * WIN, lanes] = mixed[
                    r * cols + w * WIN : r * cols + (w + 1) * WIN
                ]
    mixed = mixed_ref[...]
    hidden = layer_norm(mixed, gain1_ref[...])
    projected = jnp.dot(hidden, in_ref[...], preferred_element_type=f32)
    member = member_matrix(channels)
    groups = []
    for g in range(width // channels):
        query = projected[:, g * channels : (g + 1) * channels]
        key = projected[:, width + g * channels : width + (g + 1) * channels]
        query = query * (lax.rsqrt(head_sums(query * query, member) + unit_eps) * scale_row(scale_ref, g * (channels // HEAD), channels))
        key = key * lax.rsqrt(head_sums(key * key, member) + unit_eps)
        value = projected[:, 2 * width + g * channels : 2 * width + (g + 1) * channels].astype(bf16)
        groups.append((jnp.concatenate(halves(query), axis=-1), *halves(key), value))
    heads = channels // HEAD
    head_of = lax.broadcasted_iota(jnp.int32, (area, 2 * channels), 1) % channels // HEAD
    lane_head = lax.broadcasted_iota(jnp.int32, (area, channels), 1) // HEAD
    def score_of(w, g):
        query, key_high, key_low, value = groups[g]
        span = slice(w * area, (w + 1) * area)
        q = query[span]
        spread_q = jnp.concatenate(
            [jnp.where(head_of == j, q, jnp.zeros_like(q)) for j in range(heads)], axis=0
        )
        kh = key_high[span]
        return nt_dot(jnp.concatenate([kh, kh], axis=-1), spread_q) + nt_dot(
            key_low[span], spread_q[:, :channels]
        )

    def soften(scores):
        weight = jnp.exp(scores - jnp.max(scores, axis=0, keepdims=True))
        return (weight * (1.0 / jnp.sum(weight, axis=0, keepdims=True))).astype(bf16)

    def finish(w, g, weight):
        span = slice(w * area, (w + 1) * area)
        mixed_values = lax.dot_general(weight, groups[g][3][span], (((0,), (0,)), ((), ())), preferred_element_type=f32)
        attended = mixed_values[:area]
        for j in range(1, heads):
            attended = jnp.where(lane_head == j, mixed_values[j * area : (j + 1) * area], attended)
        attended_ref[span, g * channels : (g + 1) * channels] = attended.astype(bf16)

    units = [(w, g) for w in range(windows) for g in range(len(groups))]
    all_scores = [score_of(w, g) for w, g in units]
    all_weights = [soften(s) for s in all_scores]
    for (w, g), weight in zip(units, all_weights):
        finish(w, g, weight)
    mixed = mixed + jnp.dot(attended_ref[...], out_w_ref[...], preferred_element_type=f32)
    hidden = layer_norm(mixed, gain2_ref[...])
    inner = jnp.dot(hidden, up_ref[...], preferred_element_type=f32)
    inner = (inner / (1.0 + jnp.exp(-inner))).astype(bf16)
    result = mixed + jnp.dot(inner, down_ref[...], preferred_element_type=f32)
    for r in range(height):
        for w in range(0, windows, 2):
            pair = [result[v * area + r * WIN : v * area + (r + 1) * WIN] for v in (w, w + 1)]
            out_ref[0, r, w * WIN : (w + 2) * WIN, :] = jnp.concatenate(pair, axis=0).astype(bf16)


def layer_stage(bev_maps, joined, bev_halo, joined_halo, conv_weight, gain_first, window_in, window_out,
                window_scale, gain_second, hidden_up, hidden_down):
    vehicles, height, width_cells, channels = bev_maps.shape
    width = 2 * channels
    cells = height * width_cells
    block = pl.BlockSpec((1, height, width_cells, channels), lambda i: (i, 0, 0, 0))
    edge = pl.BlockSpec((1, 1, width_cells, channels), lambda i: (i, 0, 0, 0))
    small = (conv_weight, gain_first[None], window_in, window_out, window_scale, gain_second[None],
             hidden_up, hidden_down)
    whole = lambda w: pl.BlockSpec(w.shape, lambda i: (0,) * w.ndim)
    scalars = pl.BlockSpec(memory_space=pltpu.SMEM)
    return pl.pallas_call(
        layer_kernel,
        grid=(vehicles,),
        in_specs=[block, block, edge, edge, edge, edge]
        + [scalars if w is window_scale else whole(w) for w in small],
        out_specs=pl.BlockSpec((1, height, width_cells, width), lambda i: (i, 0, 0, 0)),
        out_shape=jax.ShapeDtypeStruct((vehicles, height, width_cells, width), bf16),
        scratch_shapes=[pltpu.VMEM((cells, width), f32), pltpu.VMEM((cells, width), bf16)],
        compiler_params=pltpu.CompilerParams(dimension_semantics=("arbitrary",)),
        name="layer_stage",
    )(bev_maps, joined, *bev_halo, *joined_halo, *small)


RING = 8
PLANE = 8
HOPS = (0, -1, 1, -2, 2, -3, 3, 4)
PIECES = 2
SHARES = 2
SLOTS = 2


def join_kernel(vehicle_ref, tile_ref, slot_ref, bias_ref, scale_ref, maps_ref, query_ref, keyvalue_ref,
                out_w_ref, joined_ref, bev_up, bev_down, joined_up, joined_down, *scratch):
    (ring_send, ring_recv, plane_send, plane_recv, edge_send, edge_recv, outbox) = scratch[-7:]
    inboxes = scratch[-7 - PIECES : -7]
    me = lax.axis_index("veh")
    plane, seat = me // PLANE, me % PLANE
    vehicles, height, tile_cols, _, part, channels = maps_ref.shape
    depth = vehicles // SHARES
    bands = lax.axis_size("row")
    band = lax.axis_index("row")
    below = {"row": lax.rem(band + 1, bands)}
    above = {"row": lax.rem(band + bands - 1, bands)}
    ahead = {"veh": lax.rem(plane + 1, RING) * PLANE + seat}
    behind = {"veh": lax.rem(plane + RING - 1, RING) * PLANE + seat}
    peers = [{"veh": plane * PLANE + lax.rem(seat + j, PLANE)} for j in range(PLANE)]

    barrier = pltpu.get_barrier_semaphore()
    for peer in (ahead, behind, below, above, *peers[1:]):
        pl.semaphore_signal(barrier, inc=1, device_id=peer, device_id_type=pl.DeviceIdType.MESH)
    pl.semaphore_wait(barrier, PLANE + 3)

    started = []

    def send(src, dst, send_sem, recv_sem, target):
        copy = pltpu.make_async_remote_copy(
            src_ref=src,
            dst_ref=dst,
            send_sem=send_sem,
            recv_sem=recv_sem,
            device_id=target,
            device_id_type=pl.DeviceIdType.MESH,
        )
        copy.start()
        return copy

    def settle(ref, sem):
        pltpu.make_async_copy(ref, ref, sem).wait()

    def held(block, piece, share=None):
        span = slice(None) if share is None else pl.ds(share * depth, depth)
        if block == 0:
            return maps_ref.at[span, :, :, piece]
        return scratch[(block - 1) * PIECES + piece].at[span]

    def pass_on(source, block, piece, share, target):
        sems = (ring_send.at[block - 1, piece, share], ring_recv.at[block - 1, piece, share])
        started.append(send(held(source, piece, share), held(block, piece, share), *sems, target))

    def relay(block, piece):
        front = block % 2 == 1
        for share in range(SHARES):
            settle(held(block, piece, share), ring_recv.at[block - 1, piece, share])
            if block < RING - 3:
                pass_on(block, block + 2, piece, share, ahead if front else behind)
            elif block < RING - 1 and front == (piece < PIECES // 2):
                pass_on(block, RING - 1, piece, share, ahead if front else behind)

    def hand_out(block, piece):
        source = maps_ref if block == 0 else scratch[(block - 1) * PIECES + piece]

        def pick(j, slot):
            at = (block * PLANE + j) * SLOTS + slot
            if block == 0:
                return source[vehicle_ref[at], :, tile_ref[at], piece]
            return source[vehicle_ref[at], :, tile_ref[at]]

        def fill(j, carry):
            for slot in range(SLOTS):
                outbox[piece, block, j, slot] = pick(j, slot)
            return carry

        lax.fori_loop(1, PLANE, fill, 0)
        place = (block * PLANE + seat) * SLOTS
        for j in range(1, PLANE):
            send(outbox.at[piece, block, j], inboxes[piece].at[pl.ds(place, SLOTS)], plane_send.at[piece],
                 plane_recv.at[piece], peers[j])
        for slot in range(SLOTS):
            inboxes[piece][place + slot] = pick(0, slot)

    def attend(piece, vehicle):
        flat = lambda x: x.reshape(height * part, channels)
        agents = bias_ref.shape[0] // (vehicles * tile_cols)
        count = agents + 1
        half = height * part
        cells = half * tile_cols
        member = member_matrix(channels)
        ego = jnp.concatenate([flat(maps_ref[vehicle, :, t, piece]) for t in range(tile_cols)], axis=0)
        row = lambda t, a: (vehicle * tile_cols + t) * agents + a
        sent = [
            flat(inboxes[piece][slot_ref[row(t, a)]]) for a in range(agents) for t in range(tile_cols)
        ]
        sources = jnp.concatenate([ego] + sent, axis=0)
        query = jnp.dot(ego, query_ref[...], preferred_element_type=f32)
        keyvalue = jnp.dot(sources, keyvalue_ref[...], preferred_element_type=f32).astype(bf16)
        norm = lax.rsqrt(head_sums(query * query, member) + unit_eps)
        query = query * (norm * scale_row(scale_ref, 0, channels))
        key = keyvalue[:, :channels].astype(f32)
        norms = head_sums(key * key, member)
        products = key.reshape(count, cells, channels) * query[None]
        products = head_sums(products.reshape(count * cells, channels), member)
        score = products * lax.rsqrt(norms + unit_eps)
        scores = [score[:cells]]
        for a in range(agents):
            tops = [cells * (a + 1) + half * t for t in range(tile_cols)]
            biased = [score[at : at + half] + bias_ref[row(t, a)] for t, at in enumerate(tops)]
            scores.append(jnp.concatenate(biased, axis=0))
        top = functools.reduce(jnp.maximum, scores)
        total, mix = None, None
        for a, one in enumerate(scores):
            weight = jnp.exp(one - top)
            total = weight if total is None else total + weight
            value = weight * keyvalue[a * cells : (a + 1) * cells, channels:].astype(f32)
            mix = value if mix is None else mix + value
        mix = (mix / total).astype(bf16)
        joined = jnp.dot(mix, out_w_ref[...], preferred_element_type=f32).astype(bf16)
        for t in range(tile_cols):
            joined_ref[vehicle, :, t, piece] = joined[t * half : (t + 1) * half].reshape(
                height, part, channels
            )

    def attend_span(piece, first, last):
        def one(vehicle, carry):
            attend(piece, vehicle)
            return carry

        lax.fori_loop(first, last, one, 0)

    def send_edges(piece):
        for at, (row, ref, target) in enumerate(((height - 1, joined_up, below), (0, joined_down, above))):
            src = joined_ref.at[:, row, :, piece]
            sems = (edge_send.at[1 + piece, at], edge_recv.at[1 + piece, at])
            edges.append(send(src, ref.at[:, :, piece], *sems, target))

    edges = [
        send(maps_ref.at[:, height - 1], bev_up, edge_send.at[0, 0], edge_recv.at[0, 0], below),
        send(maps_ref.at[:, 0], bev_down, edge_send.at[0, 1], edge_recv.at[0, 1], above),
    ]
    far = RING - 1
    for share in range(SHARES):
        pass_on(0, 1, 0, share, ahead)
        pass_on(0, 2, 0, share, behind)
    hand_out(0, 0)
    hand_out(0, 1)
    for block in (1, 2, 3, 4):
        relay(block, 0)
        hand_out(block, 0)
    for share in range(SHARES):
        pass_on(0, 2, 1, share, behind)
    relay(5, 0)
    for share in range(SHARES):
        pass_on(0, 1, 1, share, ahead)
    relay(6, 0)
    hand_out(5, 0)
    hand_out(6, 0)
    relay(far, 0)
    hand_out(far, 0)
    for block in (2, 4, 1):
        relay(block, 1)
        hand_out(block, 1)
    settle(inboxes[0].at[pl.ds(0, (PLANE - 1) * RING * SLOTS)], plane_recv.at[0])
    attend_span(0, 0, vehicles // 2)
    for block in (6, 3):
        relay(block, 1)
        hand_out(block, 1)
    attend_span(0, vehicles // 2, vehicles)
    send_edges(0)
    for block in (far, 5):
        relay(block, 1)
        hand_out(block, 1)
    settle(inboxes[1].at[pl.ds(0, (PLANE - 1) * RING * SLOTS)], plane_recv.at[1])
    attend_span(1, 0, vehicles)
    send_edges(1)
    for copy in started:
        copy.wait_send()
    for piece in range(PIECES):
        settle(outbox.at[piece, pl.ds(0, PLANE - 1)], plane_send.at[piece])
    for edge in edges:
        edge.wait()


def join_stage(bev_maps, picks, slots, bias, agent_query, agent_keyvalue, agent_out, agent_scale):
    vehicles, height, width_cells, channels = bev_maps.shape
    tile_cols = width_cells // TILE
    part = TILE // PIECES
    tiled = bev_maps.reshape(vehicles, height, tile_cols, PIECES, part, channels)
    edge = (vehicles,) + tiled.shape[2:]
    block = tiled.shape[:3] + tiled.shape[4:]
    scalars = pl.BlockSpec(memory_space=pltpu.SMEM)
    vectors = pl.BlockSpec(memory_space=pltpu.VMEM)
    ring = pltpu.SemaphoreType.DMA((RING - 1, PIECES, SHARES))
    per_piece = pltpu.SemaphoreType.DMA((PIECES,))
    per_edge = pltpu.SemaphoreType.DMA((1 + PIECES, 2))
    outs = pl.pallas_call(
        join_kernel,
        in_specs=[scalars] * 5 + [vectors] * 4,
        out_specs=[vectors] + [pl.BlockSpec(memory_space=pl.ANY)] * 4,
        out_shape=[jax.ShapeDtypeStruct(tiled.shape, bf16)] + [jax.ShapeDtypeStruct(edge, bf16)] * 4,
        scratch_shapes=[pltpu.VMEM(block, bf16)] * ((RING - 1) * PIECES)
        + [pltpu.VMEM((RING * PLANE * SLOTS, height, part, channels), bf16)] * PIECES
        + [ring, ring, per_piece, per_piece, per_edge, per_edge]
        + [pltpu.VMEM((PIECES, RING, PLANE, SLOTS, height, part, channels), bf16)],
        compiler_params=pltpu.CompilerParams(collective_id=0, has_side_effects=True),
        name="join_stage",
    )(picks // tile_cols, picks % tile_cols, slots.reshape(-1), bias.reshape(-1), agent_scale, tiled,
      agent_query, agent_keyvalue, agent_out)
    flat = (vehicles, 1, width_cells, channels)
    edges = [x.reshape(flat) for x in outs[1:]]
    return outs[0].reshape(bev_maps.shape), edges[:2], edges[2:]


def route(senders, shifts, counts, vehicles_here, tile_cols):
    agents = senders.shape[1]
    devices = lax.axis_size("veh")
    myself = lax.axis_index("veh")
    plane, seat = myself // PLANE, myself % PLANE
    pair_count = vehicles_here * agents
    by_block = lambda x: lax.dynamic_slice_in_dim(x.reshape(devices, -1), plane * PLANE, PLANE, axis=0)
    sender = by_block(senders)
    shift = by_block(shifts)
    live = jnp.arange(agents)[None, None, :] < by_block(counts)[:, :, None]
    live = live.reshape(PLANE, pair_count)
    tiles = jnp.where(live, tile_cols - jnp.abs(shift), 0)
    source = sender // vehicles_here
    ordinal = jnp.arange(pair_count)
    earlier = ordinal[None, :, None] > ordinal[None, None, :]
    same = source[:, :, None] == source[:, None, :]
    start = jnp.sum(jnp.where(same & earlier, tiles[:, None, :], 0), axis=2)
    base = (sender % vehicles_here) * tile_cols + jnp.maximum(shift, 0)

    hops = jnp.asarray(HOPS, jnp.int32)
    origin = (plane + hops + RING) % RING * PLANE + seat
    order = (seat + jnp.arange(PLANE)) % PLANE
    turn = (order[:, None] == jnp.arange(PLANE)[None, :]).astype(jnp.int32)
    slot = jnp.arange(SLOTS)[None, None, :, None]
    step = slot - start[None, :, None, :]
    hit = (source[None, :, None, :] == origin[:, None, None, None]) & (step >= 0)
    hit = hit & (step < tiles[None, :, None, :])
    picks = jnp.sum(jnp.where(hit, base[None, :, None, :] + step, 0), axis=3)
    picks = jnp.sum(turn[None, :, :, None] * picks[:, None, :, :], axis=2).reshape(-1)

    mine = lambda x: lax.dynamic_index_in_dim(x, seat, axis=0, keepdims=False)
    my_source, my_shift, my_start, my_live = mine(source), mine(shift), mine(start), mine(live)
    away = (my_source // PLANE - plane + RING) % RING
    rank = jnp.where(away > RING // 2, 2 * (RING - away) - 1, jnp.maximum(2 * away, 0))
    rank = jnp.where(away == RING // 2, RING - 1, rank)
    tile_step = jnp.arange(tile_cols, dtype=jnp.int32)
    shifted = tile_step[None, :] + my_shift[:, None]
    inside = (shifted >= 0) & (shifted < tile_cols) & my_live[:, None]
    slots = ((rank * PLANE + my_source % PLANE) * SLOTS + my_start)[:, None] + tile_step[None, :]
    slots = slots - jnp.maximum(-my_shift, 0)[:, None]
    slots = jnp.where(inside, slots, 0)
    per_tile = lambda x: x.reshape(vehicles_here, agents, tile_cols).transpose(0, 2, 1).reshape(-1, agents)
    return picks, per_tile(slots), per_tile(jnp.where(inside, 0.0, -1e30))


def on_device(bev_maps, senders, shifts, counts, agent_query, agent_keyvalue, agent_out, agent_scale,
              conv_weight, gain_first, window_in, window_out, window_scale, gain_second, hidden_up,
              hidden_down):
    vehicles_here, height, width_cells, channels = bev_maps.shape
    picks, slots, bias = route(senders, shifts, counts, vehicles_here, width_cells // TILE)
    joined, bev_halo, joined_halo = join_stage(bev_maps, picks, slots, bias, agent_query,
                                               agent_keyvalue, agent_out, agent_scale)
    return layer_stage(bev_maps, joined, bev_halo, joined_halo, conv_weight, gain_first, window_in,
                       window_out, window_scale, gain_second, hidden_up, hidden_down)


def solution(mesh):
    split = P("veh", "row", None, None)
    return jax.shard_map(
        on_device, mesh=mesh, in_specs=(split,) + (P(),) * 15, out_specs=split, check_vma=False
    )
```

```python
import functools
import jax
import jax.numpy as jnp
from jax import lax
from jax.experimental import pallas as pl
from jax.experimental.pallas import tpu as pltpu
from jax.sharding import PartitionSpec as P

TILE = 32
WIN = 8
HEAD = 32
norm_eps = 1e-05
unit_eps = 1e-06
f32 = jnp.float32
bf16 = jnp.bfloat16


def nt_dot(a, b):
    return lax.dot_general(a, b, (((1,), (1,)), ((), ())), preferred_element_type=f32)


def halves(x):
    high = x.astype(bf16)
    return high, (x - high.astype(f32)).astype(bf16)


def head_sums(x, member):
    return jnp.dot(jnp.concatenate(halves(x), axis=-1), member, preferred_element_type=f32)


def member_matrix(width):
    rows = lax.broadcasted_iota(jnp.int32, (2 * width, width), 0) % width // HEAD
    lanes = lax.broadcasted_iota(jnp.int32, (2 * width, width), 1) // HEAD
    return jnp.where(rows == lanes, 1.0, 0.0).astype(bf16)


def scale_row(scale_ref, first, width):
    head = lax.broadcasted_iota(jnp.int32, (1, width), 1) // HEAD
    row = jnp.full((1, width), scale_ref[first], f32)
    for j in range(1, width // HEAD):
        row = jnp.where(head == j, scale_ref[first + j], row)
    return row


def layer_norm(x, gain):
    centred = x - jnp.mean(x, axis=-1, keepdims=True)
    spread = jnp.mean(centred * centred, axis=-1, keepdims=True)
    return (centred * lax.rsqrt(spread + norm_eps) * gain).astype(bf16)


def layer_kernel(bev_ref, joined_ref, bev_up, bev_down, joined_up, joined_down, conv_ref, gain1_ref,
                 in_ref, out_w_ref, scale_ref, gain2_ref, up_ref, down_ref, out_ref,
                 mixed_ref, attended_ref):
    height, cols, channels = bev_ref.shape[1:]
    cells = height * cols
    windows = cols // WIN
    area = WIN * WIN
    width = 2 * channels
    column = lax.broadcasted_iota(jnp.int32, (cells, channels), 0) % cols
    band = lax.axis_index("row")
    has_up = jnp.where(band > 0, 1.0, 0.0)
    has_down = jnp.where(band < lax.axis_size("row") - 1, 1.0, 0.0)
    for half, (main, top, bottom) in enumerate(
        ((bev_ref, bev_up, bev_down), (joined_ref, joined_up, joined_down))
    ):
        lanes = slice(half * channels, (half + 1) * channels)
        rows = jnp.concatenate(
            [top[0].astype(f32) * has_up, main[0].astype(f32), bottom[0].astype(f32) * has_down], axis=0
        )
        sums = []
        for dj in range(3):
            taps = [conv_ref[di, dj : dj + 1, lanes] for di in range(3)]
            if dj == 1:
                taps[1] = taps[1] + 1.0
            acc = rows[0:height] * taps[0] + rows[1 : height + 1] * taps[1] + rows[2:] * taps[2]
            sums.append(acc.reshape(cells, channels))
        mixed = (
            sums[1]
            + jnp.where(column == 0, 0.0, pltpu.roll(sums[0], 1, axis=0))
            + jnp.where(column == cols - 1, 0.0, pltpu.roll(sums[2], cells - 1, axis=0))
        )
        for r in range(height):
            for w in range(windows):
                mixed_ref[w * area + r * WIN : w * area + (r + 1) * WIN, lanes] = mixed[
                    r * cols + w * WIN : r * cols + (w + 1) * WIN
                ]
    mixed = mixed_ref[...]
    hidden = layer_norm(mixed, gain1_ref[...])
    projected = jnp.dot(hidden, in_ref[...], preferred_element_type=f32)
    member = member_matrix(channels)
    groups = []
    for g in range(width // channels):
        query = projected[:, g * channels : (g + 1) * channels]
        key = projected[:, width + g * channels : width + (g + 1) * channels]
        query = query * (lax.rsqrt(head_sums(query * query, member) + unit_eps) * scale_row(scale_ref, g * (channels // HEAD), channels))
        key = key * lax.rsqrt(head_sums(key * key, member) + unit_eps)
        value = projected[:, 2 * width + g * channels : 2 * width + (g + 1) * channels].astype(bf16)
        groups.append((jnp.concatenate(halves(query), axis=-1), *halves(key), value))
    heads = channels // HEAD
    head_of = lax.broadcasted_iota(jnp.int32, (area, 2 * channels), 1) % channels // HEAD
    lane_head = lax.broadcasted_iota(jnp.int32, (area, channels), 1) // HEAD
    def score_of(w, g):
        query, key_high, key_low, value = groups[g]
        span = slice(w * area, (w + 1) * area)
        q = query[span]
        spread_q = jnp.concatenate(
            [jnp.where(head_of == j, q, jnp.zeros_like(q)) for j in range(heads)], axis=0
        )
        kh = key_high[span]
        return nt_dot(jnp.concatenate([kh, kh], axis=-1), spread_q) + nt_dot(
            key_low[span], spread_q[:, :channels]
        )

    def soften(scores):
        weight = jnp.exp(scores - jnp.max(scores, axis=0, keepdims=True))
        return (weight * (1.0 / jnp.sum(weight, axis=0, keepdims=True))).astype(bf16)

    def finish(w, g, weight):
        span = slice(w * area, (w + 1) * area)
        mixed_values = lax.dot_general(weight, groups[g][3][span], (((0,), (0,)), ((), ())), preferred_element_type=f32)
        attended = mixed_values[:area]
        for j in range(1, heads):
            attended = jnp.where(lane_head == j, mixed_values[j * area : (j + 1) * area], attended)
        attended_ref[span, g * channels : (g + 1) * channels] = attended.astype(bf16)

    units = [(w, g) for w in range(windows) for g in range(len(groups))]
    all_scores = [score_of(w, g) for w, g in units]
    all_weights = [soften(s) for s in all_scores]
    for (w, g), weight in zip(units, all_weights):
        finish(w, g, weight)
    mixed = mixed + jnp.dot(attended_ref[...], out_w_ref[...], preferred_element_type=f32)
    hidden = layer_norm(mixed, gain2_ref[...])
    inner = jnp.dot(hidden, up_ref[...], preferred_element_type=f32)
    inner = (inner / (1.0 + jnp.exp(-inner))).astype(bf16)
    result = mixed + jnp.dot(inner, down_ref[...], preferred_element_type=f32)
    for r in range(height):
        for w in range(0, windows, 2):
            pair = [result[v * area + r * WIN : v * area + (r + 1) * WIN] for v in (w, w + 1)]
            out_ref[0, r, w * WIN : (w + 2) * WIN, :] = jnp.concatenate(pair, axis=0).astype(bf16)


def layer_stage(bev_maps, joined, bev_halo, joined_halo, conv_weight, gain_first, window_in, window_out,
                window_scale, gain_second, hidden_up, hidden_down):
    vehicles, height, width_cells, channels = bev_maps.shape
    width = 2 * channels
    cells = height * width_cells
    block = pl.BlockSpec((1, height, width_cells, channels), lambda i: (i, 0, 0, 0))
    edge = pl.BlockSpec((1, 1, width_cells, channels), lambda i: (i, 0, 0, 0))
    small = (conv_weight, gain_first[None], window_in, window_out, window_scale, gain_second[None],
             hidden_up, hidden_down)
    whole = lambda w: pl.BlockSpec(w.shape, lambda i: (0,) * w.ndim)
    scalars = pl.BlockSpec(memory_space=pltpu.SMEM)
    return pl.pallas_call(
        layer_kernel,
        grid=(vehicles,),
        in_specs=[block, block, edge, edge, edge, edge]
        + [scalars if w is window_scale else whole(w) for w in small],
        out_specs=pl.BlockSpec((1, height, width_cells, width), lambda i: (i, 0, 0, 0)),
        out_shape=jax.ShapeDtypeStruct((vehicles, height, width_cells, width), bf16),
        scratch_shapes=[pltpu.VMEM((cells, width), f32), pltpu.VMEM((cells, width), bf16)],
        compiler_params=pltpu.CompilerParams(dimension_semantics=("arbitrary",)),
        name="layer_stage",
    )(bev_maps, joined, *bev_halo, *joined_halo, *small)


RING = 8
PLANE = 8
HOPS = (0, -1, 1, -2, 2, -3, 3, 4)
PIECES = 2
SHARES = 2
SLOTS = 2


def join_kernel(vehicle_ref, tile_ref, slot_ref, bias_ref, scale_ref, maps_ref, query_ref, keyvalue_ref,
                out_w_ref, joined_ref, bev_up, bev_down, joined_up, joined_down, *scratch):
    (ring_send, ring_recv, plane_send, plane_recv, edge_send, edge_recv, outbox, ego_query, ego_keyvalue,
     ego_score) = scratch[-10:]
    inboxes = scratch[-10 - PIECES : -10]
    me = lax.axis_index("veh")
    plane, seat = me // PLANE, me % PLANE
    vehicles, height, tile_cols, _, part, channels = maps_ref.shape
    depth = vehicles // SHARES
    bands = lax.axis_size("row")
    band = lax.axis_index("row")
    below = {"row": lax.rem(band + 1, bands)}
    above = {"row": lax.rem(band + bands - 1, bands)}
    ahead = {"veh": lax.rem(plane + 1, RING) * PLANE + seat}
    behind = {"veh": lax.rem(plane + RING - 1, RING) * PLANE + seat}
    peers = [{"veh": plane * PLANE + lax.rem(seat + j, PLANE)} for j in range(PLANE)]

    barrier = pltpu.get_barrier_semaphore()
    for peer in (ahead, behind, below, above, *peers[1:]):
        pl.semaphore_signal(barrier, inc=1, device_id=peer, device_id_type=pl.DeviceIdType.MESH)
    pl.semaphore_wait(barrier, PLANE + 3)

    started = []

    def send(src, dst, send_sem, recv_sem, target):
        copy = pltpu.make_async_remote_copy(
            src_ref=src,
            dst_ref=dst,
            send_sem=send_sem,
            recv_sem=recv_sem,
            device_id=target,
            device_id_type=pl.DeviceIdType.MESH,
        )
        copy.start()
        return copy

    def settle(ref, sem):
        pltpu.make_async_copy(ref, ref, sem).wait()

    def held(block, piece, share=None):
        span = slice(None) if share is None else pl.ds(share * depth, depth)
        if block == 0:
            return maps_ref.at[span, :, :, piece]
        return scratch[(block - 1) * PIECES + piece].at[span]

    def pass_on(source, block, piece, share, target):
        sems = (ring_send.at[block - 1, piece, share], ring_recv.at[block - 1, piece, share])
        started.append(send(held(source, piece, share), held(block, piece, share), *sems, target))

    def relay(block, piece):
        front = block % 2 == 1
        for share in range(SHARES):
            settle(held(block, piece, share), ring_recv.at[block - 1, piece, share])
            if block < RING - 3:
                pass_on(block, block + 2, piece, share, ahead if front else behind)
            elif block < RING - 1 and front == (piece < PIECES // 2):
                pass_on(block, RING - 1, piece, share, ahead if front else behind)

    def hand_out(block, piece):
        source = maps_ref if block == 0 else scratch[(block - 1) * PIECES + piece]

        def pick(j, slot):
            at = (block * PLANE + j) * SLOTS + slot
            if block == 0:
                return source[vehicle_ref[at], :, tile_ref[at], piece]
            return source[vehicle_ref[at], :, tile_ref[at]]

        def fill(j, carry):
            for slot in range(SLOTS):
                outbox[piece, block, j, slot] = pick(j, slot)
            return carry

        lax.fori_loop(1, PLANE, fill, 0)
        place = (block * PLANE + seat) * SLOTS
        for j in range(1, PLANE):
            send(outbox.at[piece, block, j], inboxes[piece].at[pl.ds(place, SLOTS)], plane_send.at[piece],
                 plane_recv.at[piece], peers[j])
        for slot in range(SLOTS):
            inboxes[piece][place + slot] = pick(0, slot)

    half = height * part
    cells = half * tile_cols
    flat = lambda x: x.reshape(half, channels)

    def prepare(piece, vehicle):
        member = member_matrix(channels)
        ego = jnp.concatenate([flat(maps_ref[vehicle, :, t, piece]) for t in range(tile_cols)], axis=0)
        query = jnp.dot(ego, query_ref[...], preferred_element_type=f32)
        keyvalue = jnp.dot(ego, keyvalue_ref[...], preferred_element_type=f32).astype(bf16)
        norm = lax.rsqrt(head_sums(query * query, member) + unit_eps)
        query = query * (norm * scale_row(scale_ref, 0, channels))
        key = keyvalue[:, :channels].astype(f32)
        norm = lax.rsqrt(head_sums(key * key, member) + unit_eps)
        ego_query[vehicle] = query
        ego_keyvalue[vehicle] = keyvalue[:, channels:]
        ego_score[vehicle] = head_sums(query * key, member) * norm

    def attend(piece, vehicle):
        agents = bias_ref.shape[0] // (vehicles * tile_cols)
        member = member_matrix(channels)
        row = lambda t, a: (vehicle * tile_cols + t) * agents + a
        sent = [
            flat(inboxes[piece][slot_ref[row(t, a)]]) for a in range(agents) for t in range(tile_cols)
        ]
        sources = jnp.concatenate(sent, axis=0)
        keyvalue = jnp.dot(sources, keyvalue_ref[...], preferred_element_type=f32).astype(bf16)
        key = keyvalue[:, :channels].astype(f32)
        norms = head_sums(key * key, member)
        products = key.reshape(agents, cells, channels) * ego_query[vehicle][None]
        products = head_sums(products.reshape(agents * cells, channels), member)
        score = products * lax.rsqrt(norms + unit_eps)
        scores, values = [ego_score[vehicle]], [ego_keyvalue[vehicle]]
        for a in range(agents):
            tops = [cells * a + half * t for t in range(tile_cols)]
            biased = [score[at : at + half] + bias_ref[row(t, a)] for t, at in enumerate(tops)]
            scores.append(jnp.concatenate(biased, axis=0))
            values.append(keyvalue[a * cells : (a + 1) * cells, channels:])
        top = functools.reduce(jnp.maximum, scores)
        total, mix = None, None
        for a, one in enumerate(scores):
            weight = jnp.exp(one - top)
            total = weight if total is None else total + weight
            value = weight * values[a].astype(f32)
            mix = value if mix is None else mix + value
        mix = (mix / total).astype(bf16)
        joined = jnp.dot(mix, out_w_ref[...], preferred_element_type=f32).astype(bf16)
        for t in range(tile_cols):
            joined_ref[vehicle, :, t, piece] = joined[t * half : (t + 1) * half].reshape(
                height, part, channels
            )

    def over(task, piece, first, last):
        def one(vehicle, carry):
            task(piece, vehicle)
            return carry

        lax.fori_loop(first, last, one, 0)

    def send_edges(piece, share):
        span = pl.ds(share * depth, depth)
        for at, (row, ref, target) in enumerate(((height - 1, joined_up, below), (0, joined_down, above))):
            sems = (edge_send.at[1 + piece, share, at], edge_recv.at[1 + piece, share, at])
            edges.append(send(joined_ref.at[span, row, :, piece], ref.at[span, :, piece], *sems, target))

    edges = [
        send(maps_ref.at[:, height - 1], bev_up, edge_send.at[0, 0, 0], edge_recv.at[0, 0, 0], below),
        send(maps_ref.at[:, 0], bev_down, edge_send.at[0, 0, 1], edge_recv.at[0, 0, 1], above),
    ]
    far = RING - 1
    for share in range(SHARES):
        pass_on(0, 1, 0, share, ahead)
        pass_on(0, 2, 0, share, behind)
    hand_out(0, 0)
    hand_out(0, 1)
    for block in (1, 2, 3, 4):
        relay(block, 0)
        hand_out(block, 0)
        if block in (2, 4):
            over(prepare, 0, (block - 2) // 2 * depth, block // 2 * depth)
    for share in range(SHARES):
        pass_on(0, 2, 1, share, behind)
    relay(5, 0)
    for share in range(SHARES):
        pass_on(0, 1, 1, share, ahead)
    relay(6, 0)
    hand_out(5, 0)
    hand_out(6, 0)
    relay(far, 0)
    hand_out(far, 0)
    for block in (2, 4, 1):
        relay(block, 1)
        hand_out(block, 1)
    settle(inboxes[0].at[pl.ds(0, (PLANE - 1) * RING * SLOTS)], plane_recv.at[0])
    over(attend, 0, 0, depth)
    for block in (6, 3):
        relay(block, 1)
        hand_out(block, 1)
    over(attend, 0, depth, vehicles)
    for share in range(SHARES):
        send_edges(0, share)
    for block in (far, 5):
        relay(block, 1)
        hand_out(block, 1)
    over(prepare, 1, 0, vehicles)
    settle(inboxes[1].at[pl.ds(0, (PLANE - 1) * RING * SLOTS)], plane_recv.at[1])
    for share in range(SHARES):
        over(attend, 1, share * depth, (share + 1) * depth)
        send_edges(1, share)
    for copy in started:
        copy.wait_send()
    for piece in range(PIECES):
        settle(outbox.at[piece, pl.ds(0, PLANE - 1)], plane_send.at[piece])
    for edge in edges:
        edge.wait()


def join_stage(bev_maps, picks, slots, bias, agent_query, agent_keyvalue, agent_out, agent_scale):
    vehicles, height, width_cells, channels = bev_maps.shape
    tile_cols = width_cells // TILE
    part = TILE // PIECES
    tiled = bev_maps.reshape(vehicles, height, tile_cols, PIECES, part, channels)
    edge = (vehicles,) + tiled.shape[2:]
    block = tiled.shape[:3] + tiled.shape[4:]
    scalars = pl.BlockSpec(memory_space=pltpu.SMEM)
    vectors = pl.BlockSpec(memory_space=pltpu.VMEM)
    ring = pltpu.SemaphoreType.DMA((RING - 1, PIECES, SHARES))
    per_piece = pltpu.SemaphoreType.DMA((PIECES,))
    per_edge = pltpu.SemaphoreType.DMA((1 + PIECES, SHARES, 2))
    outs = pl.pallas_call(
        join_kernel,
        in_specs=[scalars] * 5 + [vectors] * 4,
        out_specs=[vectors] + [pl.BlockSpec(memory_space=pl.ANY)] * 4,
        out_shape=[jax.ShapeDtypeStruct(tiled.shape, bf16)] + [jax.ShapeDtypeStruct(edge, bf16)] * 4,
        scratch_shapes=[pltpu.VMEM(block, bf16)] * ((RING - 1) * PIECES)
        + [pltpu.VMEM((RING * PLANE * SLOTS, height, part, channels), bf16)] * PIECES
        + [ring, ring, per_piece, per_piece, per_edge, per_edge]
        + [pltpu.VMEM((PIECES, RING, PLANE, SLOTS, height, part, channels), bf16)]
        + [pltpu.VMEM((vehicles, height * part * tile_cols, channels), t) for t in (f32, bf16, f32)],
        compiler_params=pltpu.CompilerParams(collective_id=0, has_side_effects=True),
        name="join_stage",
    )(picks // tile_cols, picks % tile_cols, slots.reshape(-1), bias.reshape(-1), agent_scale, tiled,
      agent_query, agent_keyvalue, agent_out)
    flat = (vehicles, 1, width_cells, channels)
    edges = [x.reshape(flat) for x in outs[1:]]
    return outs[0].reshape(bev_maps.shape), edges[:2], edges[2:]


def route(senders, shifts, counts, vehicles_here, tile_cols):
    agents = senders.shape[1]
    myself = lax.axis_index("veh")
    plane, seat = myself // PLANE, myself % PLANE
    pair_count = vehicles_here * agents
    rows = PLANE * vehicles_here
    by_block = lambda x: lax.dynamic_slice_in_dim(x, plane * rows, rows, axis=0).reshape(PLANE, -1)
    sender = by_block(senders)
    shift = by_block(shifts)
    live = jnp.arange(agents)[None, None, :] < by_block(counts)[:, :, None]
    live = live.reshape(PLANE, pair_count)
    tiles = jnp.where(live, tile_cols - jnp.abs(shift), 0)
    source = sender // vehicles_here
    ordinal = jnp.arange(pair_count)
    earlier = ordinal[None, :, None] > ordinal[None, None, :]
    same = source[:, :, None] == source[:, None, :]
    start = jnp.sum(jnp.where(same & earlier, tiles[:, None, :], 0), axis=2)
    base = (sender % vehicles_here) * tile_cols + jnp.maximum(shift, 0)

    hops = jnp.asarray(HOPS, jnp.int32)
    origin = (plane + hops + RING) % RING * PLANE + seat
    order = (seat + jnp.arange(PLANE)) % PLANE
    turn = (order[:, None] == jnp.arange(PLANE)[None, :]).astype(jnp.int32)
    slot = jnp.arange(SLOTS)[None, None, :, None]
    step = slot - start[None, :, None, :]
    hit = (source[None, :, None, :] == origin[:, None, None, None]) & (step >= 0)
    hit = hit & (step < tiles[None, :, None, :])
    picks = jnp.sum(jnp.where(hit, base[None, :, None, :] + step, 0), axis=3)
    picks = jnp.sum(turn[None, :, :, None] * picks[:, None, :, :], axis=2).reshape(-1)

    mine = lambda x: lax.dynamic_index_in_dim(x, seat, axis=0, keepdims=False)
    my_source, my_shift, my_start, my_live = mine(source), mine(shift), mine(start), mine(live)
    away = (my_source // PLANE - plane + RING) % RING
    rank = jnp.where(away > RING // 2, 2 * (RING - away) - 1, jnp.maximum(2 * away, 0))
    rank = jnp.where(away == RING // 2, RING - 1, rank)
    tile_step = jnp.arange(tile_cols, dtype=jnp.int32)
    shifted = tile_step[None, :] + my_shift[:, None]
    inside = (shifted >= 0) & (shifted < tile_cols) & my_live[:, None]
    slots = ((rank * PLANE + my_source % PLANE) * SLOTS + my_start)[:, None] + tile_step[None, :]
    slots = slots - jnp.maximum(-my_shift, 0)[:, None]
    slots = jnp.where(inside, slots, 0)
    per_tile = lambda x: x.reshape(vehicles_here, agents, tile_cols).transpose(0, 2, 1).reshape(-1, agents)
    return picks, per_tile(slots), per_tile(jnp.where(inside, 0.0, -1e30))


def on_device(bev_maps, senders, shifts, counts, agent_query, agent_keyvalue, agent_out, agent_scale,
              conv_weight, gain_first, window_in, window_out, window_scale, gain_second, hidden_up,
              hidden_down):
    vehicles_here, height, width_cells, channels = bev_maps.shape
    picks, slots, bias = route(senders, shifts, counts, vehicles_here, width_cells // TILE)
    joined, bev_halo, joined_halo = join_stage(bev_maps, picks, slots, bias, agent_query,
                                               agent_keyvalue, agent_out, agent_scale)
    return layer_stage(bev_maps, joined, bev_halo, joined_halo, conv_weight, gain_first, window_in,
                       window_out, window_scale, gain_second, hidden_up, hidden_down)


def solution(mesh):
    split = P("veh", "row", None, None)
    return jax.shard_map(
        on_device, mesh=mesh, in_specs=(split,) + (P(),) * 15, out_specs=split, check_vma=False
    )
```

```python
import functools
import jax
import jax.numpy as jnp
from jax import lax
from jax.experimental import pallas as pl
from jax.experimental.pallas import tpu as pltpu
from jax.sharding import PartitionSpec as P

TILE = 32
WIN = 8
HEAD = 32
norm_eps = 1e-05
unit_eps = 1e-06
f32 = jnp.float32
bf16 = jnp.bfloat16


def nt_dot(a, b):
    return lax.dot_general(a, b, (((1,), (1,)), ((), ())), preferred_element_type=f32)


def halves(x):
    high = x.astype(bf16)
    return high, (x - high.astype(f32)).astype(bf16)


def head_sums(x, member):
    return jnp.dot(jnp.concatenate(halves(x), axis=-1), member, preferred_element_type=f32)


def member_matrix(width):
    rows = lax.broadcasted_iota(jnp.int32, (2 * width, width), 0) % width // HEAD
    lanes = lax.broadcasted_iota(jnp.int32, (2 * width, width), 1) // HEAD
    return jnp.where(rows == lanes, 1.0, 0.0).astype(bf16)


def scale_row(scale_ref, first, width):
    head = lax.broadcasted_iota(jnp.int32, (1, width), 1) // HEAD
    row = jnp.full((1, width), scale_ref[first], f32)
    for j in range(1, width // HEAD):
        row = jnp.where(head == j, scale_ref[first + j], row)
    return row


def layer_norm(x, gain):
    centred = x - jnp.mean(x, axis=-1, keepdims=True)
    spread = jnp.mean(centred * centred, axis=-1, keepdims=True)
    return (centred * lax.rsqrt(spread + norm_eps) * gain).astype(bf16)


def layer_kernel(bev_ref, joined_ref, bev_up, bev_down, joined_up, joined_down, conv_ref, gain1_ref,
                 in_ref, out_w_ref, scale_ref, gain2_ref, up_ref, down_ref, out_ref,
                 mixed_ref, attended_ref):
    height, cols, channels = bev_ref.shape[1:]
    cells = height * cols
    windows = cols // WIN
    area = WIN * WIN
    width = 2 * channels
    column = lax.broadcasted_iota(jnp.int32, (cells, channels), 0) % cols
    band = lax.axis_index("row")
    has_up = jnp.where(band > 0, 1.0, 0.0)
    has_down = jnp.where(band < lax.axis_size("row") - 1, 1.0, 0.0)
    for half, (main, top, bottom) in enumerate(
        ((bev_ref, bev_up, bev_down), (joined_ref, joined_up, joined_down))
    ):
        lanes = slice(half * channels, (half + 1) * channels)
        rows = jnp.concatenate(
            [top[0].astype(f32) * has_up, main[0].astype(f32), bottom[0].astype(f32) * has_down], axis=0
        )
        sums = []
        for dj in range(3):
            taps = [conv_ref[di, dj : dj + 1, lanes] for di in range(3)]
            if dj == 1:
                taps[1] = taps[1] + 1.0
            acc = rows[0:height] * taps[0] + rows[1 : height + 1] * taps[1] + rows[2:] * taps[2]
            sums.append(acc.reshape(cells, channels))
        mixed = (
            sums[1]
            + jnp.where(column == 0, 0.0, pltpu.roll(sums[0], 1, axis=0))
            + jnp.where(column == cols - 1, 0.0, pltpu.roll(sums[2], cells - 1, axis=0))
        )
        for r in range(height):
            for w in range(windows):
                mixed_ref[w * area + r * WIN : w * area + (r + 1) * WIN, lanes] = mixed[
                    r * cols + w * WIN : r * cols + (w + 1) * WIN
                ]
    mixed = mixed_ref[...]
    hidden = layer_norm(mixed, gain1_ref[...])
    projected = jnp.dot(hidden, in_ref[...], preferred_element_type=f32)
    member = member_matrix(channels)
    groups = []
    for g in range(width // channels):
        query = projected[:, g * channels : (g + 1) * channels]
        key = projected[:, width + g * channels : width + (g + 1) * channels]
        query = query * (lax.rsqrt(head_sums(query * query, member) + unit_eps) * scale_row(scale_ref, g * (channels // HEAD), channels))
        key = key * lax.rsqrt(head_sums(key * key, member) + unit_eps)
        value = projected[:, 2 * width + g * channels : 2 * width + (g + 1) * channels].astype(bf16)
        groups.append((jnp.concatenate(halves(query), axis=-1), *halves(key), value))
    heads = channels // HEAD
    head_of = lax.broadcasted_iota(jnp.int32, (area, 2 * channels), 1) % channels // HEAD
    lane_head = lax.broadcasted_iota(jnp.int32, (area, channels), 1) // HEAD
    def score_of(w, g):
        query, key_high, key_low, value = groups[g]
        span = slice(w * area, (w + 1) * area)
        q = query[span]
        spread_q = jnp.concatenate(
            [jnp.where(head_of == j, q, jnp.zeros_like(q)) for j in range(heads)], axis=0
        )
        kh = key_high[span]
        return nt_dot(jnp.concatenate([kh, kh], axis=-1), spread_q) + nt_dot(
            key_low[span], spread_q[:, :channels]
        )

    def soften(scores):
        weight = jnp.exp(scores - jnp.max(scores, axis=0, keepdims=True))
        return (weight * (1.0 / jnp.sum(weight, axis=0, keepdims=True))).astype(bf16)

    def finish(w, g, weight):
        span = slice(w * area, (w + 1) * area)
        mixed_values = lax.dot_general(weight, groups[g][3][span], (((0,), (0,)), ((), ())), preferred_element_type=f32)
        attended = mixed_values[:area]
        for j in range(1, heads):
            attended = jnp.where(lane_head == j, mixed_values[j * area : (j + 1) * area], attended)
        attended_ref[span, g * channels : (g + 1) * channels] = attended.astype(bf16)

    units = [(w, g) for g in range(len(groups)) for w in range(windows)]
    all_scores = [score_of(w, g) for w, g in units]
    all_weights = [soften(s) for s in all_scores]
    for (w, g), weight in zip(units, all_weights):
        finish(w, g, weight)
    mixed = mixed + jnp.dot(attended_ref[...], out_w_ref[...], preferred_element_type=f32)
    hidden = layer_norm(mixed, gain2_ref[...])
    inner = jnp.dot(hidden, up_ref[...], preferred_element_type=f32)
    inner = (inner / (1.0 + jnp.exp(-inner))).astype(bf16)
    result = mixed + jnp.dot(inner, down_ref[...], preferred_element_type=f32)
    for r in range(height):
        for w in range(0, windows, 2):
            pair = [result[v * area + r * WIN : v * area + (r + 1) * WIN] for v in (w, w + 1)]
            out_ref[0, r, w * WIN : (w + 2) * WIN, :] = jnp.concatenate(pair, axis=0).astype(bf16)


def layer_stage(bev_maps, joined, bev_halo, joined_halo, conv_weight, gain_first, window_in, window_out,
                window_scale, gain_second, hidden_up, hidden_down):
    vehicles, height, width_cells, channels = bev_maps.shape
    width = 2 * channels
    cells = height * width_cells
    block = pl.BlockSpec((1, height, width_cells, channels), lambda i: (i, 0, 0, 0))
    edge = pl.BlockSpec((1, 1, width_cells, channels), lambda i: (i, 0, 0, 0))
    small = (conv_weight, gain_first[None], window_in, window_out, window_scale, gain_second[None],
             hidden_up, hidden_down)
    whole = lambda w: pl.BlockSpec(w.shape, lambda i: (0,) * w.ndim)
    scalars = pl.BlockSpec(memory_space=pltpu.SMEM)
    return pl.pallas_call(
        layer_kernel,
        grid=(vehicles,),
        in_specs=[block, block, edge, edge, edge, edge]
        + [scalars if w is window_scale else whole(w) for w in small],
        out_specs=pl.BlockSpec((1, height, width_cells, width), lambda i: (i, 0, 0, 0)),
        out_shape=jax.ShapeDtypeStruct((vehicles, height, width_cells, width), bf16),
        scratch_shapes=[pltpu.VMEM((cells, width), f32), pltpu.VMEM((cells, width), bf16)],
        compiler_params=pltpu.CompilerParams(dimension_semantics=("arbitrary",)),
        name="layer_stage",
    )(bev_maps, joined, *bev_halo, *joined_halo, *small)


RING = 8
PLANE = 8
HOPS = (0, -1, 1, -2, 2, -3, 3, 4)
PIECES = 2
SHARES = 2
SLOTS = 2


def join_kernel(vehicle_ref, tile_ref, slot_ref, bias_ref, scale_ref, maps_ref, query_ref, keyvalue_ref,
                out_w_ref, joined_ref, bev_up, bev_down, joined_up, joined_down, *scratch):
    (ring_send, ring_recv, plane_send, plane_recv, edge_send, edge_recv, outbox, ego_query, ego_keyvalue,
     ego_score) = scratch[-10:]
    inboxes = scratch[-10 - PIECES : -10]
    me = lax.axis_index("veh")
    plane, seat = me // PLANE, me % PLANE
    vehicles, height, tile_cols, _, part, channels = maps_ref.shape
    depth = vehicles // SHARES
    bands = lax.axis_size("row")
    band = lax.axis_index("row")
    below = {"row": lax.rem(band + 1, bands)}
    above = {"row": lax.rem(band + bands - 1, bands)}
    ahead = {"veh": lax.rem(plane + 1, RING) * PLANE + seat}
    behind = {"veh": lax.rem(plane + RING - 1, RING) * PLANE + seat}
    peers = [{"veh": plane * PLANE + lax.rem(seat + j, PLANE)} for j in range(PLANE)]

    barrier = pltpu.get_barrier_semaphore()
    for peer in (ahead, behind, below, above, *peers[1:]):
        pl.semaphore_signal(barrier, inc=1, device_id=peer, device_id_type=pl.DeviceIdType.MESH)
    pl.semaphore_wait(barrier, PLANE + 3)

    started = []

    def send(src, dst, send_sem, recv_sem, target):
        copy = pltpu.make_async_remote_copy(
            src_ref=src,
            dst_ref=dst,
            send_sem=send_sem,
            recv_sem=recv_sem,
            device_id=target,
            device_id_type=pl.DeviceIdType.MESH,
        )
        copy.start()
        return copy

    def settle(ref, sem):
        pltpu.make_async_copy(ref, ref, sem).wait()

    def held(block, piece, share=None):
        span = slice(None) if share is None else pl.ds(share * depth, depth)
        if block == 0:
            return maps_ref.at[span, :, :, piece]
        return scratch[(block - 1) * PIECES + piece].at[span]

    def pass_on(source, block, piece, share, target):
        sems = (ring_send.at[block - 1, piece, share], ring_recv.at[block - 1, piece, share])
        started.append(send(held(source, piece, share), held(block, piece, share), *sems, target))

    def relay(block, piece):
        front = block % 2 == 1
        for share in range(SHARES):
            settle(held(block, piece, share), ring_recv.at[block - 1, piece, share])
            if block < RING - 3:
                pass_on(block, block + 2, piece, share, ahead if front else behind)
            elif block < RING - 1 and front == (piece < PIECES // 2):
                pass_on(block, RING - 1, piece, share, ahead if front else behind)

    def hand_out(block, piece):
        source = maps_ref if block == 0 else scratch[(block - 1) * PIECES + piece]

        def pick(j, slot):
            at = (block * PLANE + j) * SLOTS + slot
            if block == 0:
                return source[vehicle_ref[at], :, tile_ref[at], piece]
            return source[vehicle_ref[at], :, tile_ref[at]]

        def fill(j, carry):
            for slot in range(SLOTS):
                outbox[piece, block, j, slot] = pick(j, slot)
            return carry

        lax.fori_loop(1, PLANE, fill, 0)
        place = (block * PLANE + seat) * SLOTS
        for j in range(1, PLANE):
            send(outbox.at[piece, block, j], inboxes[piece].at[pl.ds(place, SLOTS)], plane_send.at[piece],
                 plane_recv.at[piece], peers[j])
        for slot in range(SLOTS):
            inboxes[piece][place + slot] = pick(0, slot)

    half = height * part
    cells = half * tile_cols
    flat = lambda x: x.reshape(half, channels)

    def prepare(piece, vehicle):
        member = member_matrix(channels)
        ego = jnp.concatenate([flat(maps_ref[vehicle, :, t, piece]) for t in range(tile_cols)], axis=0)
        query = jnp.dot(ego, query_ref[...], preferred_element_type=f32)
        keyvalue = jnp.dot(ego, keyvalue_ref[...], preferred_element_type=f32).astype(bf16)
        norm = lax.rsqrt(head_sums(query * query, member) + unit_eps)
        query = query * (norm * scale_row(scale_ref, 0, channels))
        key = keyvalue[:, :channels].astype(f32)
        norm = lax.rsqrt(head_sums(key * key, member) + unit_eps)
        ego_query[vehicle] = query
        ego_keyvalue[vehicle] = keyvalue[:, channels:]
        ego_score[vehicle] = head_sums(query * key, member) * norm

    def attend(piece, vehicle):
        agents = bias_ref.shape[0] // (vehicles * tile_cols)
        member = member_matrix(channels)
        row = lambda t, a: (vehicle * agents + a) * tile_cols + t
        sent = [
            flat(inboxes[piece][slot_ref[row(t, a)]]) for a in range(agents) for t in range(tile_cols)
        ]
        sources = jnp.concatenate(sent, axis=0)
        keyvalue = jnp.dot(sources, keyvalue_ref[...], preferred_element_type=f32).astype(bf16)
        key = keyvalue[:, :channels].astype(f32)
        norms = head_sums(key * key, member)
        products = key.reshape(agents, cells, channels) * ego_query[vehicle][None]
        products = head_sums(products.reshape(agents * cells, channels), member)
        score = products * lax.rsqrt(norms + unit_eps)
        scores, values = [ego_score[vehicle]], [ego_keyvalue[vehicle]]
        for a in range(agents):
            tops = [cells * a + half * t for t in range(tile_cols)]
            biased = [score[at : at + half] + bias_ref[row(t, a)] for t, at in enumerate(tops)]
            scores.append(jnp.concatenate(biased, axis=0))
            values.append(keyvalue[a * cells : (a + 1) * cells, channels:])
        top = functools.reduce(jnp.maximum, scores)
        total, mix = None, None
        for a, one in enumerate(scores):
            weight = jnp.exp(one - top)
            total = weight if total is None else total + weight
            value = weight * values[a].astype(f32)
            mix = value if mix is None else mix + value
        mix = (mix / total).astype(bf16)
        joined = jnp.dot(mix, out_w_ref[...], preferred_element_type=f32).astype(bf16)
        for t in range(tile_cols):
            joined_ref[vehicle, :, t, piece] = joined[t * half : (t + 1) * half].reshape(
                height, part, channels
            )

    def over(task, piece, first, last):
        def one(vehicle, carry):
            task(piece, vehicle)
            return carry

        lax.fori_loop(first, last, one, 0)

    def send_edges(piece, share):
        span = pl.ds(share * depth, depth)
        for at, (row, ref, target) in enumerate(((height - 1, joined_up, below), (0, joined_down, above))):
            sems = (edge_send.at[1 + piece, share, at], edge_recv.at[1 + piece, share, at])
            edges.append(send(joined_ref.at[span, row, :, piece], ref.at[span, :, piece], *sems, target))

    edges = [
        send(maps_ref.at[:, height - 1], bev_up, edge_send.at[0, 0, 0], edge_recv.at[0, 0, 0], below),
        send(maps_ref.at[:, 0], bev_down, edge_send.at[0, 0, 1], edge_recv.at[0, 0, 1], above),
    ]
    far = RING - 1
    for share in range(SHARES):
        pass_on(0, 1, 0, share, ahead)
        pass_on(0, 2, 0, share, behind)
    hand_out(0, 0)
    hand_out(0, 1)
    for block in (1, 2, 3, 4):
        relay(block, 0)
        hand_out(block, 0)
        if block in (2, 4):
            over(prepare, 0, (block - 2) // 2 * depth, block // 2 * depth)
    for share in range(SHARES):
        pass_on(0, 2, 1, share, behind)
    relay(5, 0)
    for share in range(SHARES):
        pass_on(0, 1, 1, share, ahead)
    relay(6, 0)
    hand_out(5, 0)
    hand_out(6, 0)
    relay(far, 0)
    hand_out(far, 0)
    for block in (2, 4, 1):
        relay(block, 1)
        hand_out(block, 1)
    settle(inboxes[0].at[pl.ds(0, (PLANE - 1) * RING * SLOTS)], plane_recv.at[0])
    over(attend, 0, 0, depth)
    for block in (6, 3):
        relay(block, 1)
        hand_out(block, 1)
    over(attend, 0, depth, vehicles)
    for share in range(SHARES):
        send_edges(0, share)
    for block in (far, 5):
        relay(block, 1)
        hand_out(block, 1)
    over(prepare, 1, 0, vehicles)
    settle(inboxes[1].at[pl.ds(0, (PLANE - 1) * RING * SLOTS)], plane_recv.at[1])
    for share in range(SHARES):
        over(attend, 1, share * depth, (share + 1) * depth)
        send_edges(1, share)
    for copy in started:
        copy.wait_send()
    for piece in range(PIECES):
        settle(outbox.at[piece, pl.ds(0, PLANE - 1)], plane_send.at[piece])
    for edge in edges:
        edge.wait()


def join_stage(bev_maps, picks, slots, bias, agent_query, agent_keyvalue, agent_out, agent_scale):
    vehicles, height, width_cells, channels = bev_maps.shape
    tile_cols = width_cells // TILE
    part = TILE // PIECES
    tiled = bev_maps.reshape(vehicles, height, tile_cols, PIECES, part, channels)
    edge = (vehicles,) + tiled.shape[2:]
    block = tiled.shape[:3] + tiled.shape[4:]
    scalars = pl.BlockSpec(memory_space=pltpu.SMEM)
    vectors = pl.BlockSpec(memory_space=pltpu.VMEM)
    ring = pltpu.SemaphoreType.DMA((RING - 1, PIECES, SHARES))
    per_piece = pltpu.SemaphoreType.DMA((PIECES,))
    per_edge = pltpu.SemaphoreType.DMA((1 + PIECES, SHARES, 2))
    outs = pl.pallas_call(
        join_kernel,
        in_specs=[scalars] * 5 + [vectors] * 4,
        out_specs=[vectors] + [pl.BlockSpec(memory_space=pl.ANY)] * 4,
        out_shape=[jax.ShapeDtypeStruct(tiled.shape, bf16)] + [jax.ShapeDtypeStruct(edge, bf16)] * 4,
        scratch_shapes=[pltpu.VMEM(block, bf16)] * ((RING - 1) * PIECES)
        + [pltpu.VMEM((RING * PLANE * SLOTS, height, part, channels), bf16)] * PIECES
        + [ring, ring, per_piece, per_piece, per_edge, per_edge]
        + [pltpu.VMEM((PIECES, RING, PLANE, SLOTS, height, part, channels), bf16)]
        + [pltpu.VMEM((vehicles, height * part * tile_cols, channels), t) for t in (f32, bf16, f32)],
        compiler_params=pltpu.CompilerParams(collective_id=0, has_side_effects=True),
        name="join_stage",
    )(picks // tile_cols, picks % tile_cols, slots.reshape(-1), bias.reshape(-1), agent_scale, tiled,
      agent_query, agent_keyvalue, agent_out)
    flat = (vehicles, 1, width_cells, channels)
    edges = [x.reshape(flat) for x in outs[1:]]
    return outs[0].reshape(bev_maps.shape), edges[:2], edges[2:]


def route(senders, shifts, counts, vehicles_here, tile_cols):
    agents = senders.shape[1]
    myself = lax.axis_index("veh")
    plane, seat = myself // PLANE, myself % PLANE
    pair_count = vehicles_here * agents
    rows = PLANE * vehicles_here
    by_block = lambda x: lax.dynamic_slice_in_dim(x, plane * rows, rows, axis=0).reshape(PLANE, -1)
    sender = by_block(senders)
    shift = by_block(shifts)
    live = jnp.arange(agents)[None, None, :] < by_block(counts)[:, :, None]
    live = live.reshape(PLANE, pair_count)
    tiles = jnp.where(live, tile_cols - jnp.abs(shift), 0)
    source = sender // vehicles_here
    ordinal = jnp.arange(pair_count)
    earlier = ordinal[None, :, None] > ordinal[None, None, :]
    same = source[:, :, None] == source[:, None, :]
    start = jnp.sum(jnp.where(same & earlier, tiles[:, None, :], 0), axis=2)
    base = (sender % vehicles_here) * tile_cols + jnp.maximum(shift, 0)

    hops = jnp.asarray(HOPS, jnp.int32)
    origin = (plane + hops + RING) % RING * PLANE + seat
    order = (seat + jnp.arange(PLANE)) % PLANE
    turn = (order[:, None] == jnp.arange(PLANE)[None, :]).astype(jnp.int32)
    slot = jnp.arange(SLOTS)[None, None, :, None]
    step = slot - start[None, :, None, :]
    hit = (source[None, :, None, :] == origin[:, None, None, None]) & (step >= 0)
    hit = hit & (step < tiles[None, :, None, :])
    picks = jnp.sum(jnp.where(hit, base[None, :, None, :] + step, 0), axis=3)
    picks = jnp.sum(turn[None, :, :, None] * picks[:, None, :, :], axis=2).reshape(-1)

    mine = lambda x: lax.dynamic_index_in_dim(x, seat, axis=0, keepdims=False)
    my_source, my_shift, my_start, my_live = mine(source), mine(shift), mine(start), mine(live)
    away = (my_source // PLANE - plane + RING) % RING
    rank = jnp.where(away > RING // 2, 2 * (RING - away) - 1, jnp.maximum(2 * away, 0))
    rank = jnp.where(away == RING // 2, RING - 1, rank)
    tile_step = jnp.arange(tile_cols, dtype=jnp.int32)
    shifted = tile_step[None, :] + my_shift[:, None]
    inside = (shifted >= 0) & (shifted < tile_cols) & my_live[:, None]
    slots = ((rank * PLANE + my_source % PLANE) * SLOTS + my_start)[:, None] + tile_step[None, :]
    slots = slots - jnp.maximum(-my_shift, 0)[:, None]
    slots = jnp.where(inside, slots, 0)
    return picks, slots, jnp.where(inside, 0.0, -1e30)


def on_device(bev_maps, senders, shifts, counts, agent_query, agent_keyvalue, agent_out, agent_scale,
              conv_weight, gain_first, window_in, window_out, window_scale, gain_second, hidden_up,
              hidden_down):
    vehicles_here, height, width_cells, channels = bev_maps.shape
    picks, slots, bias = route(senders, shifts, counts, vehicles_here, width_cells // TILE)
    joined, bev_halo, joined_halo = join_stage(bev_maps, picks, slots, bias, agent_query,
                                               agent_keyvalue, agent_out, agent_scale)
    return layer_stage(bev_maps, joined, bev_halo, joined_halo, conv_weight, gain_first, window_in,
                       window_out, window_scale, gain_second, hidden_up, hidden_down)


def solution(mesh):
    split = P("veh", "row", None, None)
    return jax.shard_map(
        on_device, mesh=mesh, in_specs=(split,) + (P(),) * 15, out_specs=split, check_vma=False
    )
```
